32 devices in a mesh: group: 4 (over y, x), dev: 8 (over z, core).
Axes of the slice: x: 2, y: 2, z: 4, core: 2. Of those that a mesh axis runs over, the one named last changes fastest.
Arguments:
- grid_state: bfloat16 [32768, 512], P(('group', 'dev')), may hold values from -6 to 6
- mesh_state: bfloat16 [4096, 512], P(('group', 'dev')), may hold values from -6 to 6
- encode_edge: bfloat16 [512, 512], replicated, may hold values from -0.25 to 0.25
- encode_first: bfloat16 [512, 512], replicated, may hold values from -0.25 to 0.25
- encode_second: bfloat16 [512, 512], replicated, may hold values from -0.25 to 0.25
- process_edge: bfloat16 [512, 512], replicated, may hold values from -0.25 to 0.25
- process_first: bfloat16 [512, 512], replicated, may hold values from -0.25 to 0.25
- process_second: bfloat16 [512, 512], replicated, may hold values from -0.25 to 0.25
- decode_edge: bfloat16 [512, 512], replicated, may hold values from -0.25 to 0.25
- decode_first: bfloat16 [512, 512], replicated, may hold values from -0.25 to 0.25
- decode_second: bfloat16 [512, 512], replicated, may hold values from -0.25 to 0.25
- encode_near: bfloat16 [3, 4096, 1024], P(None, ('group', 'dev')), may hold values from -0.09375 to 0.09375
- encode_live: int32 [3, 256], P(None, ('group', 'dev')), may hold values 0 or 1
- encode_far: bfloat16 [2, 4096, 1024], P(None, ('group', 'dev')), may hold values from -0.09375 to 0.09375
- encode_groups: int32 [2, 32], P(None, ('group', 'dev')), may hold values from 0 to 3, as said below
- process_near: bfloat16 [3, 4096, 128], P(None, ('group', 'dev')), may hold values from -0.25 to 0.25
- process_far: bfloat16 [2, 4096, 128], P(None, ('group', 'dev')), may hold values from -0.25 to 0.25
- process_groups: int32 [2, 32], P(None, ('group', 'dev')), may hold values from 0 to 3, as said below
- decode_near: bfloat16 [3, 32768, 128], P(None, ('group', 'dev')), may hold values from -0.3125 to 0.3125
- decode_live: int32 [3, 256], P(None, ('group', 'dev')), may hold values 0 or 1
Outputs:
- grid_next: bfloat16 [32768, 512], P(('group', 'dev'))
- mesh_next: bfloat16 [4096, 512], P(('group', 'dev'))
The draws below stay inside these ranges and needn't reach their ends.
Inputs may be any that keep to these rules, and one draw needn't show every extreme that they name: `encode_groups`: for each device q the 2 entries of column q are distinct regions, none equal to q's own region q // 8. `process_groups`: for each device q the 2 entries of column q are distinct regions, none equal to q's own region q // 8.
All inputs are finite; a program needn't handle non-finite values. No bound on the sum of `encode_live` or of `decode_live` on one device may be relied on, other than what follows from the above.
Results may differ from the reference program's by a relative error of at most 0.013.
Values may be sent and summed in bfloat16 or wider, within the bound.
A program may use at most 64 MiB of HBM per device.

```python
import jax
import jax.numpy as jnp
from jax import lax

D = 512
TILE = 128
GRID_DEV = 1024
LONG = 2
TILES_DEV = 8
GRID_NODES = 32768
MESH_NODES = 4096
N_GROUP = 4
N_DEV = 8
DEVICES = 32


def far_regions(key):
    total_devices = N_GROUP * N_DEV
    scores = jax.random.randint(key, (total_devices, N_GROUP - 1), 0, 1 << 20) * N_GROUP
    scores = scores + jnp.arange(N_GROUP - 1, dtype=jnp.int32)[None, :]
    chosen = jnp.argsort(scores, axis=1, stable=True)[:, :LONG].astype(jnp.int32)
    own_group = jnp.arange(total_devices, dtype=jnp.int32) // N_DEV
    return ((own_group[:, None] + 1 + chosen) % N_GROUP).T.astype(jnp.int32)


def draw_encode_groups(key, part):
    return far_regions(jax.random.fold_in(key, 11))


def draw_process_groups(key, part):
    return far_regions(jax.random.fold_in(key, 23))


def place_ends(result, own_key, least, high):
    place = [jax.random.randint(jax.random.fold_in(own_key, axis), (), 0, length) for axis, length in enumerate(result.shape)]
    main_axis = result.shape.index(max(result.shape))
    next_to = place[:main_axis] + [(place[main_axis] + 1) % result.shape[main_axis]] + place[main_axis + 1:]
    return result.at[tuple(place)].set(least).at[tuple(next_to)].set(high)


def block_levels(own_key, extent, shards, smallest, largest):
    loudness, own = 1.0, jax.random.fold_in(own_key, 6)
    for axis_at, parts in shards:
        draws = jnp.exp(jax.random.uniform(jax.random.fold_in(own, axis_at), (parts,), jnp.float32, smallest / len(shards), largest / len(shards)))
        loudness = loudness * jnp.repeat(draws, extent[axis_at] // parts).reshape([-1 if axis == axis_at else 1 for axis in range(len(extent))])
    return loudness


def normal_values(stream_key, dims, spread, limit, pieces=(), kind=jnp.bfloat16):
    array = jax.random.normal(stream_key, dims, jnp.float32) * spread
    if len(pieces) > 0:
        array = block_levels(stream_key, dims, pieces, -0.22, 0.18) * array
    return jnp.clip(array, min=-limit, max=limit).astype(kind)


def setup_inputs(seed: int = 0) -> dict:
    key_of = jax.random.split(jax.random.key(seed), 21)
    return {
        "grid_state": normal_values(key_of[0], (GRID_NODES, D), 1.0, 6.0, ((0, 32),)),
        "mesh_state": normal_values(key_of[1], (MESH_NODES, D), 1.0, 6.0, ((0, 32),)),
        "encode_edge": normal_values(key_of[2], (D, D), D ** -0.5, 0.25),
        "encode_first": normal_values(key_of[3], (D, D), D ** -0.5, 0.25),
        "encode_second": normal_values(key_of[4], (D, D), D ** -0.5, 0.25),
        "process_edge": normal_values(key_of[5], (D, D), D ** -0.5, 0.25),
        "process_first": normal_values(key_of[6], (D, D), D ** -0.5, 0.25),
        "process_second": normal_values(key_of[7], (D, D), D ** -0.5, 0.25),
        "decode_edge": normal_values(key_of[8], (D, D), D ** -0.5, 0.25),
        "decode_first": normal_values(key_of[9], (D, D), D ** -0.5, 0.25),
        "decode_second": normal_values(key_of[10], (D, D), D ** -0.5, 0.25),
        "encode_near": normal_values(key_of[11], (3, MESH_NODES, GRID_DEV), (4 * GRID_DEV) ** -0.5, 0.09375, ((1, 32),)),
        "encode_live": place_ends((jax.random.randint(key_of[12], (3, TILES_DEV * DEVICES), 0, 3) < 2).astype(jnp.int32), jax.random.fold_in(key_of[12], 1), 0, 1),
        "encode_far": normal_values(key_of[13], (LONG, MESH_NODES, GRID_DEV), (4 * GRID_DEV) ** -0.5, 0.09375, ((1, 32),)),
        "encode_groups": draw_encode_groups(jax.random.fold_in(key_of[20], 71), 0),
        "process_near": normal_values(key_of[15], (3, MESH_NODES, TILE), (5 * TILE) ** -0.5, 0.25, ((1, 32),)),
        "process_far": normal_values(key_of[16], (LONG, MESH_NODES, TILE), (5 * TILE) ** -0.5, 0.25, ((1, 32),)),
        "process_groups": draw_process_groups(jax.random.fold_in(key_of[20], 71), 0),
        "decode_near": normal_values(key_of[18], (3, GRID_NODES, TILE), (3 * TILE) ** -0.5, 0.3125, ((1, 32),)),
        "decode_live": place_ends((jax.random.randint(key_of[19], (3, TILES_DEV * DEVICES), 0, 3) < 2).astype(jnp.int32), jax.random.fold_in(key_of[19], 1), 0, 1),
    }


highest = lax.Precision.HIGHEST

def layer_norm(row_values):
    row_mean = lax.optimization_barrier(jnp.mean(row_values, axis=-1, keepdims=True))
    centred = row_values - row_mean
    variance = lax.optimization_barrier(jnp.mean(centred * centred, axis=-1, keepdims=True))
    return centred * lax.rsqrt(variance + 1e-05)

def node_update(residual_in, summed, weight_in, weight_out):
    normed = layer_norm(summed).astype(jnp.bfloat16)
    hidden = jax.nn.silu(jnp.dot(normed, weight_in, preferred_element_type=jnp.float32)).astype(jnp.bfloat16)
    updated = residual_in.astype(jnp.float32) + jnp.dot(hidden, weight_out, preferred_element_type=jnp.float32)
    return updated.astype(jnp.bfloat16)

def edge_messages(latents, weight):
    return jax.nn.silu(jnp.dot(latents, weight, preferred_element_type=jnp.float32)).astype(jnp.bfloat16)

def shift_blocks(stacked):
    empty = jnp.zeros_like(stacked[:, :1])
    from_below = jnp.concatenate([empty, stacked[:, :-1]], axis=1)
    from_above = jnp.concatenate([stacked[:, 1:], empty], axis=1)
    return (from_below, from_above)

def reference(grid_state, mesh_state, encode_edge, encode_first, encode_second, process_edge, process_first, process_second, decode_edge, decode_first, decode_second, encode_near, encode_live, encode_far, encode_groups, process_near, process_far, process_groups, decode_near, decode_live):
    enc_msg = edge_messages(grid_state, encode_edge).reshape(N_GROUP, N_DEV, GRID_DEV, D)
    live_enc = encode_live.reshape(3, N_GROUP, N_DEV, TILES_DEV).transpose(1, 0, 2, 3)
    near_enc = encode_near.reshape(3, N_GROUP, N_DEV, TILE, GRID_DEV).transpose(1, 0, 2, 3, 4)
    far_enc = encode_far.reshape(LONG, N_GROUP, N_DEV, TILE, GRID_DEV).transpose(1, 0, 2, 3, 4)

    def group_sources(inputs):
        messages, live_flags, near_tiles, far_tiles = inputs
        wide = messages.astype(jnp.float32)
        near_out = []
        for offset in range(3):
            flags = jnp.repeat(live_flags[offset].astype(jnp.float32), TILE, axis=1)
            masked = wide * flags[:, :, None]
            product = jnp.einsum('dtr,drk->dtk', near_tiles[offset].astype(jnp.float32), masked, precision=highest)
            near_out.append(product.astype(jnp.bfloat16))
        far_out = []
        for index in range(LONG):
            product = jnp.einsum('dtr,drk->dtk', far_tiles[index].astype(jnp.float32), wide, precision=highest)
            far_out.append(product.astype(jnp.bfloat16))
        return (jnp.stack(near_out), jnp.stack(far_out))
    near_part, far_part = lax.map(group_sources, (enc_msg, live_enc, near_enc, far_enc))
    near_wide = near_part.astype(jnp.float32)
    from_below, from_above = shift_blocks(near_wide[:, 2])
    above_part = jnp.concatenate([near_wide[:, 0, 1:], jnp.zeros_like(near_wide[:, 0, :1])], axis=1)
    enc_sum = near_wide[:, 1] + from_below + above_part
    groups_enc = encode_groups.reshape(LONG, N_GROUP, N_DEV)
    select_enc = (groups_enc[..., None] == jnp.arange(N_GROUP, dtype=jnp.int32)).astype(jnp.float32)
    enc_sum = enc_sum + jnp.einsum('lgdh,gldtk->hdtk', select_enc, far_part.astype(jnp.float32), precision=highest)
    mesh_mid = node_update(mesh_state, enc_sum.reshape(MESH_NODES, D), encode_first, encode_second)
    proc_msg = edge_messages(mesh_mid, process_edge).reshape(N_GROUP, N_DEV, TILE, D).astype(jnp.float32)
    below_msg, above_msg = shift_blocks(proc_msg)
    near_proc = process_near.reshape(3, N_GROUP, N_DEV, TILE, TILE).astype(jnp.float32)
    proc_sum = jnp.einsum('gdij,gdjk->gdik', near_proc[0], below_msg, precision=highest)
    proc_sum = proc_sum + jnp.einsum('gdij,gdjk->gdik', near_proc[1], proc_msg, precision=highest)
    proc_sum = proc_sum + jnp.einsum('gdij,gdjk->gdik', near_proc[2], above_msg, precision=highest)
    groups_proc = process_groups.reshape(LONG, N_GROUP, N_DEV)
    select_proc = (groups_proc[..., None] == jnp.arange(N_GROUP, dtype=jnp.int32)).astype(jnp.float32)
    picked = jnp.einsum('lgdh,hdjk->lgdjk', select_proc, proc_msg, precision=highest)
    far_proc = process_far.reshape(LONG, N_GROUP, N_DEV, TILE, TILE).astype(jnp.float32)
    proc_sum = proc_sum + jnp.einsum('lgdij,lgdjk->gdik', far_proc, picked, precision=highest)
    mesh_next = node_update(mesh_mid, proc_sum.reshape(MESH_NODES, D), process_first, process_second)
    dec_msg = edge_messages(mesh_next, decode_edge).reshape(N_GROUP, N_DEV, TILE, D)
    dec_below, dec_above = shift_blocks(dec_msg)
    near_dec = decode_near.reshape(3, N_GROUP, N_DEV, GRID_DEV, TILE).transpose(1, 0, 2, 3, 4)
    live_dec = decode_live.reshape(3, N_GROUP, N_DEV, TILES_DEV).transpose(1, 0, 2, 3)
    grid_groups = grid_state.reshape(N_GROUP, N_DEV * GRID_DEV, D)

    def group_decode(inputs):
        below_blk, own_blk, above_blk, near_tiles, live_flags, grid_rows = inputs
        sources = (below_blk, own_blk, above_blk)
        summed = jnp.zeros((N_DEV, GRID_DEV, D), jnp.float32)
        for offset in range(3):
            product = jnp.einsum('dri,dik->drk', near_tiles[offset].astype(jnp.float32), sources[offset].astype(jnp.float32), precision=highest)
            flags = jnp.repeat(live_flags[offset].astype(jnp.float32), TILE, axis=1)
            summed = summed + product * flags[:, :, None]
        return node_update(grid_rows, summed.reshape(N_DEV * GRID_DEV, D), decode_first, decode_second)
    grid_next = lax.map(group_decode, (dec_below, dec_msg, dec_above, near_dec, live_dec, grid_groups))
    return (grid_next.reshape(GRID_NODES, D), mesh_next)
```

```python
import contextlib
import functools

import jax
import jax.numpy as jnp
from jax import lax
from jax.experimental import pallas as pl
from jax.experimental.pallas import tpu as pltpu
from jax.sharding import PartitionSpec as P

BF16 = jnp.bfloat16
F32 = jnp.float32
CHUNKS = 2
GRID_LOADS = 2
GRID_OUTS = 4


def silu(x):
    half = 0.5 * x
    return half + half * jnp.tanh(half)


def mm(a, b):
    return jnp.dot(a, b, preferred_element_type=F32)


def layer_norm(v):
    mean = jnp.mean(v, axis=-1, keepdims=True)
    cent = v - mean
    var = jnp.mean(cent * cent, axis=-1, keepdims=True)
    return cent * lax.rsqrt(var + 1e-05)


def partner(me, r, count):
    if count & (count - 1):
        return lax.rem(me + r, count), lax.rem(me + count - r, count)
    out, bit = me, 1
    while bit < count:
        if r & bit:
            out = out + bit * (1 - 2 * lax.rem(me // bit, 2))
        bit *= 2
    return out, out


def scope(name):
    return contextlib.nullcontext()


def exchange(
    groups,
    devs,
    grid_h, mesh_h, ee_h, e1_h, e2_h, pe_h, p1_h, p2_h, de_h, d1_h, d2_h,
    en_h, el_h, ef_h, eg_h, pn_h, pf_h, pg_h, dn_h, dl_h,
    mesh_out, gs, dw, acc,
    ms, wt, inc, live, regions, pinc, dn,
    em, fheld, fsend, frelay, frecv, nsend, nrecv, msend, mfrecv, mnrecv, dsend, dnrecv,
    own_near, proc_inc,
    load_sem, grid_sem, fs_sem, fl_sem, fr_sem, ns_sem, nr_sem, mfs_sem, mfl_sem, mfr_sem, mns_sem, mnr_sem, ds_sem, dr_sem,
):
    g = lax.axis_index("group")
    d = lax.axis_index("dev")
    rows, feats = ms.shape
    width = feats // CHUNKS
    far_count = groups - 1
    long_count = pinc.shape[0] - 3
    tiles = live.shape[2]
    peers = [partner(g, r, groups) for r in range(1, groups)]
    order = list(reversed(range(far_count)))
    relay = groups == 4
    halves = fsend.shape[2]
    piece_rows = rows // halves
    if relay:
        greeted = [to for to, _ in peers[:2]]
    elif groups & (groups - 1):
        greeted = [to for to, _ in peers] + [source for _, source in peers]
    else:
        greeted = [to for to, _ in peers]
    not_first, not_last = d > 0, d < devs - 1
    sides = ((not_first, d - 1), (not_last, d + 1))
    near_side = 1 - lax.rem(d, 2)

    def load(index, pairs, whole):
        starts = [pltpu.make_async_copy(src, dst, load_sem.at[index]) for src, dst in pairs]
        return starts, pltpu.make_async_copy(whole, whole, load_sem.at[index])

    far_inc, near_inc = inc.at[pl.ds(0, long_count)], inc.at[pl.ds(long_count, 3)]
    first = load(0, [(ee_h, wt.at[0])], wt.at[0])
    far_load = load(1, [(ef_h, far_inc)], far_inc)
    near_load = load(2, [(en_h, near_inc)], near_inc)
    live_load = load(3, [(el_h, live.at[0]), (dl_h, live.at[1])], live)
    region_load = load(4, [(eg_h, regions.at[0]), (pg_h, regions.at[1])], regions)
    late = [
        load(5, [(mesh_h, ms)], ms),
        load(6, [(e1_h, wt.at[1]), (e2_h, wt.at[2]), (pe_h, wt.at[3])], wt.at[pl.ds(1, 3)]),
        load(7, [(pn_h, pinc.at[pl.ds(0, 3)]), (pf_h, pinc.at[pl.ds(3, long_count)])], pinc),
        load(8, [(dn_h, dn)], dn),
        load(9, [(p1_h, wt.at[4]), (p2_h, wt.at[5]), (de_h, wt.at[6])], wt.at[pl.ds(4, 3)]),
        load(10, [(d1_h, dw.at[0]), (d2_h, dw.at[1])], dw),
    ]

    def start_load(loads):
        for copy in loads[0]:
            copy.start()

    step = gs.shape[0] // grid_sem.shape[0]
    count = gs.shape[0] // step
    grid_loads = [
        pltpu.make_async_copy(grid_h.at[pl.ds(i * step, step)], gs.at[pl.ds(i * step, step)], grid_sem.at[i])
        for i in range(count)
    ]
    start_load(first)
    for copy in grid_loads:
        copy.start()
    for loads in (region_load, far_load, live_load, near_load):
        start_load(loads)

    barrier = pltpu.get_barrier_semaphore()
    for to in greeted:
        pl.semaphore_signal(barrier, inc=1, device_id=(to, d), device_id_type=pl.DeviceIdType.MESH)
    for there, near in sides:
        @pl.when(there)
        def _():
            pl.semaphore_signal(barrier, inc=1, device_id=(g, near), device_id_type=pl.DeviceIdType.MESH)

    for side, (there, _) in enumerate(sides):
        @pl.when(jnp.logical_not(there))
        def _():
            for buf in (nrecv, mnrecv, dnrecv):
                for c in range(CHUNKS):
                    buf[side, c] = jnp.zeros((rows, width), BF16)

    def remote(src, dst, send, recv, to):
        return pltpu.make_async_remote_copy(
            src_ref=src, dst_ref=dst, send_sem=send, recv_sem=recv, device_id=to, device_id_type=pl.DeviceIdType.MESH
        )

    def whole(ref, send, recv):
        return remote(ref, ref, send, recv, (peers[0][0], d))

    def first_axis(h):
        return h % 2

    def far_copy(c, h, kind):
        if not relay:
            return remote(fsend.at[c, kind, h], frecv.at[c, kind, h], fs_sem.at[0], fr_sem.at[c], (peers[kind][0], d))
        to = first_axis(h) if kind < 2 else 1 - first_axis(h)
        if kind == 0:
            return remote(fsend.at[c, 0, h], frelay.at[c, h], fs_sem.at[0], fl_sem.at[c, h], (peers[to][0], d))
        return remote(fsend.at[c, kind, h], frecv.at[c, kind - 1, h], fs_sem.at[0], fr_sem.at[c], (peers[to][0], d))

    def near_copy(c, s):
        return remote(nsend.at[s, c], nrecv.at[1 - s, c], ns_sem.at[s], nr_sem.at[1 - s], (g, sides[s][1]))

    def mfar_copy(c, h, i):
        at = pl.ds(h * piece_rows, piece_rows)
        source, to, recv = msend.at[c, at], i, mfr_sem.at[c, 0]
        if relay:
            if i == 2:
                source, to, recv = mfrecv.at[c, first_axis(h), at], 1 - first_axis(h), mfr_sem.at[c, 1]
            elif i == first_axis(h):
                recv = mfl_sem.at[c, h]
        return remote(source, mfrecv.at[c, i, at], mfs_sem.at[0], recv, (peers[to][0], d))

    def mnear_copy(c, s):
        return remote(msend.at[c], mnrecv.at[1 - s, c], mns_sem.at[s], mnr_sem.at[1 - s], (g, sides[s][1]))

    def dec_copy(c, s):
        return remote(dsend.at[c], dnrecv.at[1 - s, c], ds_sem.at[s], dr_sem.at[1 - s, c], (g, sides[s][1]))

    def start_side(copy, c):
        for s, (there, _) in enumerate(sides):
            @pl.when(there)
            def _():
                copy(c, s).start()

    def wait_side(buf, sem, s):
        @pl.when(sides[s][0])
        def _():
            whole(buf.at[s], sem.at[s], sem.at[s]).wait_recv()

    with scope("ldwait"):
        first[1].wait()
    for c in range(CHUNKS):
        cols = pl.ds(c * width, width)
        for i in range(count):
            if c == 0:
                with scope("gridwait"):
                    grid_loads[i].wait()
            at = pl.ds(i * step, step)
            em[c, at, :] = silu(mm(gs[at, :], wt[0, :, cols])).astype(BF16)
        if c == 0:
            for loads in late:
                start_load(loads)
            with scope("efwait"):
                region_load[1].wait()
                far_load[1].wait()
        far_all = mm(inc[pl.ds(0, long_count)].reshape(long_count * rows, gs.shape[0]), em[c])
        far = [far_all[i * rows:(i + 1) * rows] for i in range(long_count)]

        def toward(i):
            total = None
            for index in range(long_count):
                flag = jnp.where(regions[0, 0, index] == peers[i][0], 1.0, 0.0).astype(F32)
                term = far[index] * flag
                total = term if total is None else total + term
            return total

        if c == 0:
            with scope("barrier"):
                pl.semaphore_wait(barrier, len(greeted) + jnp.where(not_first, 1, 0) + jnp.where(not_last, 1, 0))
        if relay:
            totals = [toward(i) for i in range(far_count)]
            for kind in range(2):
                for h in range(halves):
                    at = slice(h * piece_rows, (h + 1) * piece_rows)
                    axis = first_axis(h)
                    fsend[c, kind, h] = totals[2 if kind == 0 else axis][at].astype(BF16)
                    far_copy(c, h, kind).start()
                    if kind == 0:
                        fheld[c, h] = totals[1 - axis][at]
        else:
            for i in order:
                fsend[c, i, 0] = toward(i).astype(BF16)
                far_copy(c, 0, i).start()

    with scope("enwait"):
        live_load[1].wait()
        near_load[1].wait()
    for k in range(3):
        for t in range(tiles):
            flag = live[0, k, t].astype(F32).astype(BF16)
            at = pl.ds(t * rows, rows)
            inc[long_count + k, :, at] = inc[long_count + k, :, at] * flag
    for c in range(CHUNKS):
        cols = pl.ds(c * width, width)
        near_all = mm(inc[pl.ds(long_count, 3)].reshape(3 * rows, gs.shape[0]), em[c])
        for s, k in ((0, 0), (1, 2)):
            nsend[s, c] = near_all[k * rows:(k + 1) * rows].astype(BF16)
        start_side(near_copy, c)
        own_near[:, cols] = near_all[rows:2 * rows].astype(BF16)

    if relay:
        for c in range(CHUNKS):
            for h in range(halves):
                with scope("relaywait"):
                    far_copy(c, h, 0).wait_recv()
                fsend[c, 2, h] = (fheld[c, h] + frelay[c, h].astype(F32)).astype(BF16)
                far_copy(c, h, 2).start()

    for loads in late:
        loads[1].wait()
    for i in range(far_count):
        total = None
        for index in range(long_count):
            flag = jnp.where(regions[1, 0, index] == peers[i][1], 1.0, 0.0).astype(F32)
            term = pinc[3 + index].astype(F32) * flag
            total = term if total is None else total + term
        proc_inc[i] = total.astype(BF16)
    for k in range(3):
        for t in range(tiles):
            at = pl.ds(t * rows, rows)
            dn[k, at, :] = dn[k, at, :] * live[1, k, t].astype(F32).astype(BF16)

    def node_update(residual, summed, first, second):
        hidden = silu(mm(layer_norm(summed).astype(BF16), wt[first])).astype(BF16)
        return (residual.astype(F32) + mm(hidden, wt[second])).astype(BF16)

    with scope("nearwait"):
        for s in range(2):
            wait_side(nrecv, nr_sem, s)
    parts = []
    for c in range(CHUNKS):
        total = own_near[:, pl.ds(c * width, width)].astype(F32)
        for s in range(2):
            total = total + nrecv[s, c].astype(F32)
        with scope("farwait"):
            whole(frecv.at[c], fr_sem.at[c], fr_sem.at[c]).wait_recv()
        pieces = []
        for h in range(halves):
            piece = total[h * piece_rows:(h + 1) * piece_rows]
            for i in range(frecv.shape[1]):
                piece = piece + frecv[c, i, h].astype(F32)
            pieces.append(piece)
        parts.append(jnp.concatenate(pieces, axis=0))
    with scope("upd1"):
        mesh_mid = node_update(ms[...], jnp.concatenate(parts, axis=1), 1, 2)

    for c in range(CHUNKS):
        msend[c] = silu(mm(mesh_mid, wt[3, :, pl.ds(c * width, width)])).astype(BF16)
        if not relay:
            for i in order:
                mfar_copy(c, 0, i).start()
        else:
            for h in range(halves):
                mfar_copy(c, h, first_axis(h)).start()
        start_side(mnear_copy, c)
    if relay:
        for c in range(CHUNKS):
            for h in range(halves):
                mfar_copy(c, h, 1 - first_axis(h)).start()
    parts = [mm(pinc[1], msend[c]) for c in range(CHUNKS)]
    if relay:
        for c in range(CHUNKS):
            for h in range(halves):
                with scope("mrelaywait"):
                    mfar_copy(c, h, first_axis(h)).wait_recv()
                mfar_copy(c, h, 2).start()
    for s in range(2):
        with scope("mnearwait"):
            wait_side(mnrecv, mnr_sem, s)
        for c in range(CHUNKS):
            parts[c] = parts[c] + mm(pinc[2 * s], mnrecv[s, c])
    for c in range(CHUNKS):
        with scope("mfarwait"):
            if relay:
                whole(mfrecv.at[c, 0], mfr_sem.at[c, 0], mfr_sem.at[c, 0]).wait_recv()
            else:
                whole(mfrecv.at[c], mfr_sem.at[c, 0], mfr_sem.at[c, 0]).wait_recv()
        for i in range(2 if relay else far_count):
            parts[c] = parts[c] + mm(proc_inc[i], mfrecv[c, i])
    if relay:
        for c in range(CHUNKS):
            with scope("mdiagwait"):
                whole(mfrecv.at[c, 2], mfr_sem.at[c, 1], mfr_sem.at[c, 1]).wait_recv()
            parts[c] = parts[c] + mm(proc_inc[2], mfrecv[c, 2])
    with scope("upd2"):
        mesh_next = node_update(mesh_mid, jnp.concatenate(parts, axis=1), 4, 5)
    mesh_out[...] = mesh_next

    for c in range(CHUNKS):
        dsend[c] = silu(mm(mesh_next, wt[6, :, pl.ds(c * width, width)])).astype(BF16)
        start_side(dec_copy, c)

    block = 2 * rows

    def decode(add, c, k, source):
        for i in range(gs.shape[0] // block):
            at = pl.ds(i * block, block)
            part = mm(dn[k, at, :], source)
            acc[at, pl.ds(c * width, width)] = acc[at, pl.ds(c * width, width)] + part if add else part

    with scope("ownpart"):
        for c in range(CHUNKS):
            decode(False, c, 1, dsend[c])
    for s in (near_side, 1 - near_side):
        there = jnp.where(s == 0, not_first, not_last)
        for c in range(CHUNKS):
            with scope("decwait"):
                @pl.when(there)
                def _():
                    whole(dnrecv.at[s, c], dr_sem.at[s, c], dr_sem.at[s, c]).wait_recv()
            decode(True, c, 2 * s, dnrecv[s, c])

    with scope("drain"):
        whole(fsend, fs_sem.at[0], fs_sem.at[0]).wait_send()
        whole(mfrecv, mfs_sem.at[0], mfs_sem.at[0]).wait_send()
        for s, (there, _) in enumerate(sides):
            @pl.when(there)
            def _():
                whole(nsend.at[s], ns_sem.at[s], ns_sem.at[s]).wait_send()
                whole(msend, mns_sem.at[s], mns_sem.at[s]).wait_send()
                whole(dsend, ds_sem.at[s], ds_sem.at[s]).wait_send()


def finish(mesh_v, gs, dw, acc, grid_o, mesh_o, grid_out, out_sem):
    step = gs.shape[0] // (out_sem.shape[0] - 1)
    mesh_copy = pltpu.make_async_copy(mesh_v, mesh_o, out_sem.at[0])
    mesh_copy.start()
    outs = []
    for i in range(gs.shape[0] // step):
        at = pl.ds(i * step, step)
        hidden = silu(mm(layer_norm(acc[at, :]).astype(BF16), dw[0])).astype(BF16)
        grid_out[at, :] = (gs[at, :].astype(F32) + mm(hidden, dw[1])).astype(BF16)
        copy = pltpu.make_async_copy(grid_out.at[at], grid_o.at[at], out_sem.at[1 + i])
        copy.start()
        outs.append(copy)
    with scope("outwait"):
        mesh_copy.wait()
        for copy in outs:
            copy.wait()


def body(groups, devs, *args):
    grid_state, mesh_state = args[0], args[1]
    args = list(args)
    args[14], args[17] = args[14].T, args[17].T
    encode_live, encode_far, encode_groups, decode_near = args[12], args[13], args[14], args[18]
    grid_rows, feats = grid_state.shape
    rows = mesh_state.shape[0]
    width = feats // CHUNKS
    far_count = groups - 1
    long_count = encode_far.shape[0]

    def vmem(*shape, dtype=BF16):
        return pltpu.VMEM(shape, dtype)

    dma = pltpu.SemaphoreType.DMA
    relay = groups == 4
    halves = 2 if relay else 1
    piece = (rows // halves, width)
    block = (rows, width)
    scratch = [
        vmem(rows, feats), vmem(7, feats, feats), vmem(3 + long_count, rows, grid_rows),
        pltpu.SMEM((2, *encode_live.shape), jnp.int32), pltpu.SMEM((2, *encode_groups.shape), jnp.int32),
        vmem(3 + long_count, rows, rows), vmem(*decode_near.shape),
        vmem(CHUNKS, grid_rows, width),
        vmem(CHUNKS, halves, *piece, dtype=F32), vmem(CHUNKS, far_count, halves, *piece),
        vmem(CHUNKS, halves, *piece), vmem(CHUNKS, 2 if relay else far_count, halves, *piece),
        vmem(2, CHUNKS, *block), vmem(2, CHUNKS, *block),
        vmem(CHUNKS, *block), vmem(CHUNKS, far_count, *block), vmem(2, CHUNKS, *block),
        vmem(CHUNKS, *block), vmem(2, CHUNKS, *block),
        vmem(rows, feats), vmem(far_count, rows, rows),
        dma((11,)), dma((GRID_LOADS,)), dma((1,)), dma((CHUNKS, halves)), dma((CHUNKS,)), dma((2,)), dma((2,)),
        dma((1,)), dma((CHUNKS, halves)), dma((CHUNKS, halves)), dma((2,)), dma((2,)), dma((2,)), dma((2, CHUNKS)),
    ]
    hbm = pl.BlockSpec(memory_space=pltpu.HBM)
    on_chip = pl.BlockSpec(memory_space=pltpu.VMEM)
    held = pl.pallas_call(
        functools.partial(exchange, groups, devs),
        out_shape=(
            vmem(*mesh_state.shape), vmem(*grid_state.shape), vmem(2, feats, feats), vmem(*grid_state.shape, dtype=F32),
        ),
        in_specs=[hbm] * len(args),
        out_specs=(on_chip,) * 4,
        scratch_shapes=scratch,
        compiler_params=pltpu.CompilerParams(collective_id=0, has_side_effects=True, vmem_limit_bytes=32 << 20),
        name="exchange",
    )(*(pltpu.with_memory_space_constraint(arg, pltpu.HBM) for arg in args))
    return pl.pallas_call(
        finish,
        out_shape=(
            jax.ShapeDtypeStruct(grid_state.shape, BF16),
            jax.ShapeDtypeStruct(mesh_state.shape, BF16),
        ),
        in_specs=[on_chip] * 4,
        out_specs=(hbm, hbm),
        scratch_shapes=[vmem(*grid_state.shape), dma((1 + GRID_OUTS,))],
        compiler_params=pltpu.CompilerParams(vmem_limit_bytes=16 << 20),
        name="finish",
    )(*held)


def solution(mesh):
    both = ("group", "dev")
    row, whole, second = P(both, None), P(), P(None, both, None)
    flags = P(None, both)
    return jax.shard_map(
        functools.partial(body, mesh.shape["group"], mesh.shape["dev"]),
        mesh=mesh,
        in_specs=(
            row, row, whole, whole, whole, whole, whole, whole, whole, whole, whole,
            second, flags, second, flags, second, second, flags, second, flags,
        ),
        out_specs=(row, row),
        check_vma=False,
    )
```

```python
import contextlib
import functools

import jax
import jax.numpy as jnp
from jax import lax
from jax.experimental import pallas as pl
from jax.experimental.pallas import tpu as pltpu
from jax.sharding import PartitionSpec as P

BF16 = jnp.bfloat16
F32 = jnp.float32
CHUNKS = 2
GRID_LOADS = 2
GRID_OUTS = 2
DIRECT_RS = True
DIRECT_AG = True
DEFER_RS = True
DEFER_AG = False


def silu(x):
    half = 0.5 * x
    return half + half * jnp.tanh(half)


def mm(a, b):
    return jnp.dot(a, b, preferred_element_type=F32)


def layer_norm(v):
    mean = jnp.mean(v, axis=-1, keepdims=True)
    cent = v - mean
    var = jnp.mean(cent * cent, axis=-1, keepdims=True)
    return cent * lax.rsqrt(var + 1e-05)


def partner(me, r, count):
    if count & (count - 1):
        return lax.rem(me + r, count), lax.rem(me + count - r, count)
    out, bit = me, 1
    while bit < count:
        if r & bit:
            out = out + bit * (1 - 2 * lax.rem(me // bit, 2))
        bit *= 2
    return out, out


def scope(name):
    return contextlib.nullcontext()


def exchange(
    groups,
    devs,
    grid_h, mesh_h, ee_h, e1_h, e2_h, pe_h, p1_h, p2_h, de_h, d1_h, d2_h,
    en_h, el_h, ef_h, eg_h, pn_h, pf_h, pg_h, dn_h, dl_h,
    mesh_out, gs, dw, acc,
    ms, wt, inc, live, regions, pinc, dn,
    em, fheld, fsend, frelay, frecv, nsend, nrecv, msend, mfrecv, mnrecv, dsend, dnrecv,
    own_near, proc_inc,
    load_sem, grid_sem, fs_sem, fl_sem, fr_sem, ns_sem, nr_sem, mfs_sem, mfl_sem, mfr_sem, mns_sem, mnr_sem, ds_sem, dr_sem,
):
    g = lax.axis_index("group")
    d = lax.axis_index("dev")
    rows, feats = ms.shape
    width = feats // CHUNKS
    far_count = groups - 1
    long_count = pinc.shape[0] - 3
    tiles = live.shape[2]
    peers = [partner(g, r, groups) for r in range(1, groups)]
    order = list(reversed(range(far_count)))
    relay = groups == 4
    halves = fsend.shape[2]
    piece_rows = rows // halves
    if groups & (groups - 1):
        greeted = [to for to, _ in peers] + [source for _, source in peers]
    else:
        greeted = [to for to, _ in peers]
    not_first, not_last = d > 0, d < devs - 1
    sides = ((not_first, d - 1), (not_last, d + 1))
    near_side = 1 - lax.rem(d, 2)
    even, odd = lax.rem(d, 2) == 0, lax.rem(d, 2) == 1

    def load(index, pairs, whole):
        starts = [pltpu.make_async_copy(src, dst, load_sem.at[index]) for src, dst in pairs]
        return starts, pltpu.make_async_copy(whole, whole, load_sem.at[index])

    far_inc, near_inc = inc.at[pl.ds(0, long_count)], inc.at[pl.ds(long_count, 3)]
    first = load(0, [(ee_h, wt.at[0])], wt.at[0])
    far_load = load(1, [(ef_h, far_inc)], far_inc)
    near_load = load(2, [(en_h, near_inc)], near_inc)
    live_load = load(3, [(el_h, live.at[0]), (dl_h, live.at[1])], live)
    region_load = load(4, [(eg_h, regions.at[0]), (pg_h, regions.at[1])], regions)
    late = [
        load(5, [(mesh_h, ms)], ms),
        load(6, [(e1_h, wt.at[1]), (e2_h, wt.at[2]), (pe_h, wt.at[3])], wt.at[pl.ds(1, 3)]),
        load(7, [(pn_h, pinc.at[pl.ds(0, 3)]), (pf_h, pinc.at[pl.ds(3, long_count)])], pinc),
        load(8, [(dn_h, dn)], dn),
        load(9, [(p1_h, wt.at[4]), (p2_h, wt.at[5]), (de_h, wt.at[6])], wt.at[pl.ds(4, 3)]),
        load(10, [(d1_h, dw.at[0]), (d2_h, dw.at[1])], dw),
    ]

    def start_load(loads):
        for copy in loads[0]:
            copy.start()

    step = gs.shape[0] // grid_sem.shape[0]
    count = gs.shape[0] // step
    grid_loads = [
        pltpu.make_async_copy(grid_h.at[pl.ds(i * step, step)], gs.at[pl.ds(i * step, step)], grid_sem.at[i])
        for i in range(count)
    ]
    start_load(first)
    for copy in grid_loads:
        copy.start()
    for loads in (region_load, far_load, live_load, near_load):
        start_load(loads)

    barrier = pltpu.get_barrier_semaphore()
    for to in greeted:
        pl.semaphore_signal(barrier, inc=1, device_id=(to, d), device_id_type=pl.DeviceIdType.MESH)
    for there, near in sides:
        @pl.when(there)
        def _():
            pl.semaphore_signal(barrier, inc=1, device_id=(g, near), device_id_type=pl.DeviceIdType.MESH)

    for side, (there, _) in enumerate(sides):
        @pl.when(jnp.logical_not(there))
        def _():
            for buf in (nrecv, mnrecv, dnrecv):
                for c in range(CHUNKS):
                    buf[side, c] = jnp.zeros((rows, width), BF16)

    def direct_rs(c):
        return relay and DIRECT_RS and c == CHUNKS - 1

    def direct_ag(c):
        return relay and DIRECT_AG and c == CHUNKS - 1

    if relay:
        @pl.when(odd)
        def _():
            frecv[CHUNKS - 1, 2] = jnp.zeros(frecv.shape[2:], BF16)

    def remote(src, dst, send, recv, to):
        return pltpu.make_async_remote_copy(
            src_ref=src, dst_ref=dst, send_sem=send, recv_sem=recv, device_id=to, device_id_type=pl.DeviceIdType.MESH
        )

    def whole(ref, send, recv):
        return remote(ref, ref, send, recv, (peers[0][0], d))

    def first_axis(h):
        return h % 2

    def far_copy(c, h, kind):
        if not relay:
            return remote(fsend.at[c, kind, h], frecv.at[c, kind, h], fs_sem.at[0], fr_sem.at[c], (peers[kind][0], d))
        to = first_axis(h) if kind < 2 else 1 - first_axis(h)
        if kind == 0:
            return remote(fsend.at[c, 0, h], frelay.at[c, h], fs_sem.at[0], fl_sem.at[c, h], (peers[to][0], d))
        return remote(fsend.at[c, kind, h], frecv.at[c, kind - 1, h], fs_sem.at[0], fr_sem.at[c], (peers[to][0], d))

    def far_direct(c):
        return remote(fsend.at[c, 0], frecv.at[c, 2], fs_sem.at[0], fr_sem.at[c], (peers[2][0], d))

    def mfar_direct(c):
        return remote(msend.at[c], mfrecv.at[c, 2], mfs_sem.at[0], mfr_sem.at[c, 1], (peers[2][0], d))

    def near_copy(c, s):
        return remote(nsend.at[s, c], nrecv.at[1 - s, c], ns_sem.at[s], nr_sem.at[1 - s], (g, sides[s][1]))

    def mfar_copy(c, h, i):
        at = pl.ds(h * piece_rows, piece_rows)
        source, to, recv = msend.at[c, at], i, mfr_sem.at[c, 0]
        if relay:
            if i == 2:
                source, to, recv = mfrecv.at[c, first_axis(h), at], 1 - first_axis(h), mfr_sem.at[c, 1]
            elif i == first_axis(h):
                recv = mfl_sem.at[c, h]
        return remote(source, mfrecv.at[c, i, at], mfs_sem.at[0], recv, (peers[to][0], d))

    def mnear_copy(c, s):
        return remote(msend.at[c], mnrecv.at[1 - s, c], mns_sem.at[s], mnr_sem.at[1 - s], (g, sides[s][1]))

    def dec_copy(c, s):
        return remote(dsend.at[c], dnrecv.at[1 - s, c], ds_sem.at[s], dr_sem.at[1 - s, c], (g, sides[s][1]))

    def start_side(copy, c):
        for s, (there, _) in enumerate(sides):
            @pl.when(there)
            def _():
                copy(c, s).start()

    def wait_side(buf, sem, s):
        @pl.when(sides[s][0])
        def _():
            whole(buf.at[s], sem.at[s], sem.at[s]).wait_recv()

    greetings = len(greeted) + jnp.where(not_first, 1, 0) + jnp.where(not_last, 1, 0)
    with scope("ldwait"):
        first[1].wait()
    for c in range(CHUNKS):
        cols = pl.ds(c * width, width)
        for i in range(count):
            if c == 0:
                with scope("gridwait"):
                    grid_loads[i].wait()
                    if i == count - 1:
                        region_load[1].wait()
                        far_load[1].wait()
                        pl.semaphore_wait(barrier, greetings)
            at = pl.ds(i * step, step)
            em[c, at, :] = silu(mm(gs[at, :], wt[0, :, cols])).astype(BF16)
        far_all = mm(inc[pl.ds(0, long_count)].reshape(long_count * rows, gs.shape[0]), em[c])
        far = [far_all[i * rows:(i + 1) * rows] for i in range(long_count)]

        def toward(i):
            total = None
            for index in range(long_count):
                flag = jnp.where(regions[0, 0, index] == peers[i][0], 1.0, 0.0).astype(F32)
                term = far[index] * flag
                total = term if total is None else total + term
            return total

        if relay:
            totals = [toward(i) for i in range(far_count)]
            for kind in range(2):
                for h in range(halves):
                    at = slice(h * piece_rows, (h + 1) * piece_rows)
                    axis = first_axis(h)
                    fsend[c, kind, h] = totals[2 if kind == 0 else axis][at].astype(BF16)
                    if kind == 0:
                        fheld[c, h] = totals[1 - axis][at]
                        if direct_rs(c):
                            fsend[c, 2, h] = totals[1 - axis][at].astype(BF16)

            @pl.when(even)
            def _():
                if direct_rs(c):
                    far_direct(c).start()
                for kind in range(1 if direct_rs(c) else 0, 3 if direct_rs(c) else 2):
                    for h in range(halves):
                        far_copy(c, h, kind).start()

            @pl.when(odd)
            def _():
                for h in range(halves):
                    far_copy(c, h, 0).start()
                if not DEFER_RS:
                    for h in range(halves):
                        far_copy(c, h, 1).start()
                elif c == CHUNKS - 1:
                    for b in range(CHUNKS):
                        for h in range(halves):
                            far_copy(b, h, 1).start()
        else:
            for i in order:
                fsend[c, i, 0] = toward(i).astype(BF16)
                far_copy(c, 0, i).start()

    for loads in late:
        start_load(loads)
    with scope("enwait"):
        live_load[1].wait()
        near_load[1].wait()
    for k in range(3):
        for t in range(tiles):
            flag = live[0, k, t].astype(F32).astype(BF16)
            at = pl.ds(t * rows, rows)
            inc[long_count + k, :, at] = inc[long_count + k, :, at] * flag
    for c in range(CHUNKS):
        cols = pl.ds(c * width, width)
        near_all = mm(inc[pl.ds(long_count, 3)].reshape(3 * rows, gs.shape[0]), em[c])
        for s, k in ((0, 0), (1, 2)):
            nsend[s, c] = near_all[k * rows:(k + 1) * rows].astype(BF16)
        start_side(near_copy, c)
        own_near[:, cols] = near_all[rows:2 * rows].astype(BF16)

    if relay:
        def pass_on(c):
            for h in range(halves):
                with scope("relaywait"):
                    far_copy(c, h, 0).wait_recv()
                fsend[c, 2, h] = (fheld[c, h] + frelay[c, h].astype(F32)).astype(BF16)
                far_copy(c, h, 2).start()

        for c in range(CHUNKS):
            if direct_rs(c):
                @pl.when(odd)
                def _():
                    pass_on(c)
            else:
                pass_on(c)

    for loads in late:
        loads[1].wait()
    for i in range(far_count):
        total = None
        for index in range(long_count):
            flag = jnp.where(regions[1, 0, index] == peers[i][1], 1.0, 0.0).astype(F32)
            term = pinc[3 + index].astype(F32) * flag
            total = term if total is None else total + term
        proc_inc[i] = total.astype(BF16)
    for k in range(3):
        for t in range(tiles):
            at = pl.ds(t * rows, rows)
            dn[k, at, :] = dn[k, at, :] * live[1, k, t].astype(F32).astype(BF16)

    def node_update(residual, summed, first, second):
        hidden = silu(mm(layer_norm(summed).astype(BF16), wt[first])).astype(BF16)
        return (residual.astype(F32) + mm(hidden, wt[second])).astype(BF16)

    with scope("nearwait"):
        for s in range(2):
            wait_side(nrecv, nr_sem, s)
    parts = []
    for c in range(CHUNKS):
        total = own_near[:, pl.ds(c * width, width)].astype(F32)
        for s in range(2):
            total = total + nrecv[s, c].astype(F32)
        slots = 3 if direct_rs(c) else 2 if relay else far_count
        with scope("farwait"):
            if direct_rs(c):
                @pl.when(even)
                def _():
                    whole(frecv.at[c], fr_sem.at[c], fr_sem.at[c]).wait_recv()

                @pl.when(odd)
                def _():
                    whole(frecv.at[c, pl.ds(0, 2)], fr_sem.at[c], fr_sem.at[c]).wait_recv()
            else:
                whole(frecv.at[c, pl.ds(0, slots)], fr_sem.at[c], fr_sem.at[c]).wait_recv()
        pieces = []
        for h in range(halves):
            piece = total[h * piece_rows:(h + 1) * piece_rows]
            for i in range(slots):
                piece = piece + frecv[c, i, h].astype(F32)
            pieces.append(piece)
        parts.append(jnp.concatenate(pieces, axis=0))
    with scope("upd1"):
        mesh_mid = node_update(ms[...], jnp.concatenate(parts, axis=1), 1, 2)

    for c in range(CHUNKS):
        msend[c] = silu(mm(mesh_mid, wt[3, :, pl.ds(c * width, width)])).astype(BF16)
        if not relay:
            for i in order:
                mfar_copy(c, 0, i).start()
        else:
            for h in range(halves):
                mfar_copy(c, h, first_axis(h)).start()
            if direct_ag(c):
                @pl.when(even)
                def _():
                    mfar_direct(c).start()
        start_side(mnear_copy, c)

    def send_second():
        for c in range(CHUNKS):
            for h in range(halves):
                mfar_copy(c, h, 1 - first_axis(h)).start()

    if relay and DEFER_AG:
        pl.when(even)(send_second)
    elif relay:
        send_second()
    parts = [mm(pinc[1], msend[c]) for c in range(CHUNKS)]
    if relay:
        for c in range(CHUNKS):
            for h in range(halves):
                with scope("mrelaywait"):
                    mfar_copy(c, h, first_axis(h)).wait_recv()
                if direct_ag(c):
                    @pl.when(odd)
                    def _():
                        mfar_copy(c, h, 2).start()
                else:
                    mfar_copy(c, h, 2).start()
        if DEFER_AG:
            pl.when(odd)(send_second)
    for s in range(2):
        with scope("mnearwait"):
            wait_side(mnrecv, mnr_sem, s)
        for c in range(CHUNKS):
            parts[c] = parts[c] + mm(pinc[2 * s], mnrecv[s, c])
    for c in range(CHUNKS):
        with scope("mfarwait"):
            if relay:
                whole(mfrecv.at[c, 0], mfr_sem.at[c, 0], mfr_sem.at[c, 0]).wait_recv()
            else:
                whole(mfrecv.at[c], mfr_sem.at[c, 0], mfr_sem.at[c, 0]).wait_recv()
        for i in range(2 if relay else far_count):
            parts[c] = parts[c] + mm(proc_inc[i], mfrecv[c, i])
    if relay:
        for c in range(CHUNKS):
            with scope("mdiagwait"):
                whole(mfrecv.at[c, 2], mfr_sem.at[c, 1], mfr_sem.at[c, 1]).wait_recv()
            parts[c] = parts[c] + mm(proc_inc[2], mfrecv[c, 2])
    with scope("upd2"):
        mesh_next = node_update(mesh_mid, jnp.concatenate(parts, axis=1), 4, 5)
    mesh_out[...] = mesh_next

    for c in range(CHUNKS):
        dsend[c] = silu(mm(mesh_next, wt[6, :, pl.ds(c * width, width)])).astype(BF16)
        start_side(dec_copy, c)

    block = 2 * rows

    def decode(add, c, k, source):
        for i in range(gs.shape[0] // block):
            at = pl.ds(i * block, block)
            part = mm(dn[k, at, :], source)
            acc[at, pl.ds(c * width, width)] = acc[at, pl.ds(c * width, width)] + part if add else part

    with scope("ownpart"):
        for c in range(CHUNKS):
            decode(False, c, 1, dsend[c])
    for s in (near_side, 1 - near_side):
        there = jnp.where(s == 0, not_first, not_last)
        for c in range(CHUNKS):
            with scope("decwait"):
                @pl.when(there)
                def _():
                    whole(dnrecv.at[s, c], dr_sem.at[s, c], dr_sem.at[s, c]).wait_recv()
            decode(True, c, 2 * s, dnrecv[s, c])

    with scope("drain"):
        whole(fsend, fs_sem.at[0], fs_sem.at[0]).wait_send()
        whole(mfrecv, mfs_sem.at[0], mfs_sem.at[0]).wait_send()
        for s, (there, _) in enumerate(sides):
            @pl.when(there)
            def _():
                whole(nsend.at[s], ns_sem.at[s], ns_sem.at[s]).wait_send()
                whole(msend, mns_sem.at[s], mns_sem.at[s]).wait_send()
                whole(dsend, ds_sem.at[s], ds_sem.at[s]).wait_send()


def finish(mesh_v, gs, dw, acc, grid_o, mesh_o, grid_out, out_sem):
    step = gs.shape[0] // (out_sem.shape[0] - 1)
    width = gs.shape[1] // CHUNKS
    mesh_copy = pltpu.make_async_copy(mesh_v, mesh_o, out_sem.at[0])
    mesh_copy.start()
    outs = []
    for i in range(gs.shape[0] // step):
        at = pl.ds(i * step, step)
        normed = layer_norm(acc[at, :]).astype(BF16)
        parts = [silu(mm(normed, dw[0, :, pl.ds(c * width, width)])).astype(BF16) for c in range(CHUNKS)]
        hidden = jnp.concatenate(parts, axis=1)
        for c in range(CHUNKS):
            cols = pl.ds(c * width, width)
            grid_out[at, cols] = (gs[at, cols].astype(F32) + mm(hidden, dw[1, :, cols])).astype(BF16)
        copy = pltpu.make_async_copy(grid_out.at[at], grid_o.at[at], out_sem.at[1 + i])
        copy.start()
        outs.append(copy)
    with scope("outwait"):
        mesh_copy.wait()
        for copy in outs:
            copy.wait()


def body(groups, devs, *args):
    grid_state, mesh_state = args[0], args[1]
    args = list(args)
    args[14], args[17] = args[14].T, args[17].T
    encode_live, encode_far, encode_groups, decode_near = args[12], args[13], args[14], args[18]
    grid_rows, feats = grid_state.shape
    rows = mesh_state.shape[0]
    width = feats // CHUNKS
    far_count = groups - 1
    long_count = encode_far.shape[0]

    def vmem(*shape, dtype=BF16):
        return pltpu.VMEM(shape, dtype)

    dma = pltpu.SemaphoreType.DMA
    relay = groups == 4
    halves = 2 if relay else 1
    piece = (rows // halves, width)
    block = (rows, width)
    scratch = [
        vmem(rows, feats), vmem(7, feats, feats), vmem(3 + long_count, rows, grid_rows),
        pltpu.SMEM((2, *encode_live.shape), jnp.int32), pltpu.SMEM((2, *encode_groups.shape), jnp.int32),
        vmem(3 + long_count, rows, rows), vmem(*decode_near.shape),
        vmem(CHUNKS, grid_rows, width),
        vmem(CHUNKS, halves, *piece, dtype=F32), vmem(CHUNKS, far_count, halves, *piece),
        vmem(CHUNKS, halves, *piece), vmem(CHUNKS, far_count, halves, *piece),
        vmem(2, CHUNKS, *block), vmem(2, CHUNKS, *block),
        vmem(CHUNKS, *block), vmem(CHUNKS, far_count, *block), vmem(2, CHUNKS, *block),
        vmem(CHUNKS, *block), vmem(2, CHUNKS, *block),
        vmem(rows, feats), vmem(far_count, rows, rows),
        dma((11,)), dma((GRID_LOADS,)), dma((1,)), dma((CHUNKS, halves)), dma((CHUNKS,)), dma((2,)), dma((2,)),
        dma((1,)), dma((CHUNKS, halves)), dma((CHUNKS, halves)), dma((2,)), dma((2,)), dma((2,)), dma((2, CHUNKS)),
    ]
    hbm = pl.BlockSpec(memory_space=pltpu.HBM)
    on_chip = pl.BlockSpec(memory_space=pltpu.VMEM)
    held = pl.pallas_call(
        functools.partial(exchange, groups, devs),
        out_shape=(
            vmem(*mesh_state.shape), vmem(*grid_state.shape), vmem(2, feats, feats), vmem(*grid_state.shape, dtype=F32),
        ),
        in_specs=[hbm] * len(args),
        out_specs=(on_chip,) * 4,
        scratch_shapes=scratch,
        compiler_params=pltpu.CompilerParams(collective_id=0, has_side_effects=True, vmem_limit_bytes=32 << 20),
        name="exchange",
    )(*(pltpu.with_memory_space_constraint(arg, pltpu.HBM) for arg in args))
    return pl.pallas_call(
        finish,
        out_shape=(
            jax.ShapeDtypeStruct(grid_state.shape, BF16),
            jax.ShapeDtypeStruct(mesh_state.shape, BF16),
        ),
        in_specs=[on_chip] * 4,
        out_specs=(hbm, hbm),
        scratch_shapes=[vmem(*grid_state.shape), dma((1 + GRID_OUTS,))],
        compiler_params=pltpu.CompilerParams(vmem_limit_bytes=16 << 20),
        name="finish",
    )(*held)


def solution(mesh):
    both = ("group", "dev")
    row, whole, second = P(both, None), P(), P(None, both, None)
    flags = P(None, both)
    return jax.shard_map(
        functools.partial(body, mesh.shape["group"], mesh.shape["dev"]),
        mesh=mesh,
        in_specs=(
            row, row, whole, whole, whole, whole, whole, whole, whole, whole, whole,
            second, flags, second, flags, second, second, flags, second, flags,
        ),
        out_specs=(row, row),
        check_vma=False,
    )
```

```python
import contextlib
import functools

import jax
import jax.numpy as jnp
from jax import lax
from jax.experimental import pallas as pl
from jax.experimental.pallas import tpu as pltpu
from jax.sharding import PartitionSpec as P

BF16 = jnp.bfloat16
F32 = jnp.float32
CHUNKS = 2
GRID_LOADS = 2
GRID_OUTS = 2
DIRECT_RS = 0
DIRECT_AG = 0


def silu(x):
    half = 0.5 * x
    return half + half * jnp.tanh(half)


def mm(a, b):
    return jnp.dot(a, b, preferred_element_type=F32)


def layer_norm(v):
    mean = jnp.mean(v, axis=-1, keepdims=True)
    cent = v - mean
    var = jnp.mean(cent * cent, axis=-1, keepdims=True)
    return cent * lax.rsqrt(var + 1e-05)


def partner(me, r, count):
    if count & (count - 1):
        return lax.rem(me + r, count), lax.rem(me + count - r, count)
    out, bit = me, 1
    while bit < count:
        if r & bit:
            out = out + bit * (1 - 2 * lax.rem(me // bit, 2))
        bit *= 2
    return out, out


def scope(name):
    return contextlib.nullcontext()


def exchange(
    groups,
    devs,
    grid_h, mesh_h, ee_h, e1_h, e2_h, pe_h, p1_h, p2_h, de_h, d1_h, d2_h,
    en_h, el_h, ef_h, eg_h, pn_h, pf_h, pg_h, dn_h, dl_h,
    mesh_out, gs, dw, acc,
    ms, wt, inc, live, regions, pinc, dn,
    em, fheld, fsend, frelay, frecv, nsend, nrecv, msend, mfrecv, mnrecv, dsend, dnrecv,
    own_near, proc_inc,
    load_sem, grid_sem, fs_sem, fl_sem, fr_sem, ns_sem, nr_sem, mfs_sem, mfl_sem, mfr_sem, mns_sem, mnr_sem, ds_sem, dr_sem, turn,
):
    g = lax.axis_index("group")
    d = lax.axis_index("dev")
    rows, feats = ms.shape
    width = feats // CHUNKS
    far_count = groups - 1
    long_count = pinc.shape[0] - 3
    tiles = live.shape[2]
    peers = [partner(g, r, groups) for r in range(1, groups)]
    order = list(reversed(range(far_count)))
    relay = groups == 4
    halves = fsend.shape[2]
    piece_rows = rows // halves
    if groups & (groups - 1):
        greeted = [to for to, _ in peers] + [source for _, source in peers]
    else:
        greeted = [to for to, _ in peers]
    not_first, not_last = d > 0, d < devs - 1
    sides = ((not_first, d - 1), (not_last, d + 1))
    near_side = 1 - lax.rem(d, 2)
    even, odd = lax.rem(d, 2) == 0, lax.rem(d, 2) == 1

    def load(index, pairs, whole):
        starts = [pltpu.make_async_copy(src, dst, load_sem.at[index]) for src, dst in pairs]
        return starts, pltpu.make_async_copy(whole, whole, load_sem.at[index])

    far_inc, near_inc = inc.at[pl.ds(0, long_count)], inc.at[pl.ds(long_count, 3)]
    first = load(0, [(ee_h, wt.at[0])], wt.at[0])
    far_load = load(1, [(ef_h, far_inc)], far_inc)
    near_load = load(2, [(en_h, near_inc)], near_inc)
    live_load = load(3, [(el_h, live.at[0]), (dl_h, live.at[1])], live)
    region_load = load(4, [(eg_h, regions.at[0]), (pg_h, regions.at[1])], regions)
    late = [
        load(5, [(mesh_h, ms)], ms),
        load(6, [(e1_h, wt.at[1]), (e2_h, wt.at[2]), (pe_h, wt.at[3])], wt.at[pl.ds(1, 3)]),
        load(7, [(pn_h, pinc.at[pl.ds(0, 3)]), (pf_h, pinc.at[pl.ds(3, long_count)])], pinc),
        load(8, [(dn_h, dn)], dn),
        load(9, [(p1_h, wt.at[4]), (p2_h, wt.at[5]), (de_h, wt.at[6])], wt.at[pl.ds(4, 3)]),
        load(10, [(d1_h, dw.at[0]), (d2_h, dw.at[1])], dw),
    ]

    def start_load(loads):
        for copy in loads[0]:
            copy.start()

    step = gs.shape[0] // grid_sem.shape[0]
    count = gs.shape[0] // step
    grid_loads = [
        pltpu.make_async_copy(grid_h.at[pl.ds(i * step, step)], gs.at[pl.ds(i * step, step)], grid_sem.at[i])
        for i in range(count)
    ]
    start_load(first)
    for copy in grid_loads:
        copy.start()
    for loads in (region_load, far_load, live_load, near_load):
        start_load(loads)

    barrier = pltpu.get_barrier_semaphore()
    for to in greeted:
        pl.semaphore_signal(barrier, inc=1, device_id=(to, d), device_id_type=pl.DeviceIdType.MESH)
    for there, near in sides:
        @pl.when(there)
        def _():
            pl.semaphore_signal(barrier, inc=1, device_id=(g, near), device_id_type=pl.DeviceIdType.MESH)

    for side, (there, _) in enumerate(sides):
        @pl.when(jnp.logical_not(there))
        def _():
            for buf in (nrecv, mnrecv, dnrecv):
                for c in range(CHUNKS):
                    buf[side, c] = jnp.zeros((rows, width), BF16)

    def direct_rs(c):
        return relay and c >= DIRECT_RS

    def direct_ag(c):
        return relay and c >= DIRECT_AG

    if relay:
        @pl.when(odd)
        def _():
            for c in range(DIRECT_RS, CHUNKS):
                frecv[c, 2] = jnp.zeros(frecv.shape[2:], BF16)

    def remote(src, dst, send, recv, to):
        return pltpu.make_async_remote_copy(
            src_ref=src, dst_ref=dst, send_sem=send, recv_sem=recv, device_id=to, device_id_type=pl.DeviceIdType.MESH
        )

    def whole(ref, send, recv):
        return remote(ref, ref, send, recv, (peers[0][0], d))

    def hand_over(phase):
        @pl.when(not_last)
        def _():
            pl.semaphore_signal(turn.at[phase], inc=1, device_id=(g, d + 1), device_id_type=pl.DeviceIdType.MESH)

    def first_axis(h):
        return h % 2

    def far_copy(c, h, kind):
        if not relay:
            return remote(fsend.at[c, kind, h], frecv.at[c, kind, h], fs_sem.at[c], fr_sem.at[c], (peers[kind][0], d))
        to = first_axis(h) if kind < 2 else 1 - first_axis(h)
        if kind == 0:
            return remote(fsend.at[c, 0, h], frelay.at[c, h], fs_sem.at[c], fl_sem.at[c, h], (peers[to][0], d))
        return remote(fsend.at[c, kind, h], frecv.at[c, kind - 1, h], fs_sem.at[c], fr_sem.at[c], (peers[to][0], d))

    def far_direct(c):
        return remote(fsend.at[c, 0], frecv.at[c, 2], fs_sem.at[c], fr_sem.at[c], (peers[2][0], d))

    def mfar_direct(c):
        return remote(msend.at[c], mfrecv.at[c, 2], mfs_sem.at[c], mfr_sem.at[c, 1], (peers[2][0], d))

    def near_copy(c, s):
        return remote(nsend.at[s, c], nrecv.at[1 - s, c], ns_sem.at[s], nr_sem.at[1 - s], (g, sides[s][1]))

    def mfar_copy(c, h, i):
        at = pl.ds(h * piece_rows, piece_rows)
        source, to, recv = msend.at[c, at], i, mfr_sem.at[c, 0]
        if relay:
            if i == 2:
                source, to, recv = mfrecv.at[c, first_axis(h), at], 1 - first_axis(h), mfr_sem.at[c, 1]
            elif i == first_axis(h):
                recv = mfl_sem.at[c, h]
        return remote(source, mfrecv.at[c, i, at], mfs_sem.at[c], recv, (peers[to][0], d))

    def mnear_copy(c, s):
        return remote(msend.at[c], mnrecv.at[1 - s, c], mns_sem.at[s], mnr_sem.at[1 - s], (g, sides[s][1]))

    def dec_copy(c, s):
        return remote(dsend.at[c], dnrecv.at[1 - s, c], ds_sem.at[s], dr_sem.at[1 - s, c], (g, sides[s][1]))

    def start_side(copy, c):
        for s, (there, _) in enumerate(sides):
            @pl.when(there)
            def _():
                copy(c, s).start()

    def wait_side(buf, sem, s):
        @pl.when(sides[s][0])
        def _():
            whole(buf.at[s], sem.at[s], sem.at[s]).wait_recv()

    greetings = len(greeted) + jnp.where(not_first, 1, 0) + jnp.where(not_last, 1, 0)
    with scope("ldwait"):
        first[1].wait()
    for c in range(CHUNKS):
        cols = pl.ds(c * width, width)
        for i in range(count):
            if c == 0:
                with scope("gridwait"):
                    grid_loads[i].wait()
                    if i == count - 1:
                        region_load[1].wait()
                        far_load[1].wait()
                        pl.semaphore_wait(barrier, greetings)
            at = pl.ds(i * step, step)
            em[c, at, :] = silu(mm(gs[at, :], wt[0, :, cols])).astype(BF16)
        far_all = mm(inc[pl.ds(0, long_count)].reshape(long_count * rows, gs.shape[0]), em[c])
        far = [far_all[i * rows:(i + 1) * rows] for i in range(long_count)]

        def toward(i):
            total = None
            for index in range(long_count):
                flag = jnp.where(regions[0, 0, index] == peers[i][0], 1.0, 0.0).astype(F32)
                term = far[index] * flag
                total = term if total is None else total + term
            return total

        if relay:
            totals = [toward(i) for i in range(far_count)]
            for kind in range(2):
                for h in range(halves):
                    at = slice(h * piece_rows, (h + 1) * piece_rows)
                    axis = first_axis(h)
                    fsend[c, kind, h] = totals[2 if kind == 0 else axis][at].astype(BF16)
                    if kind == 0:
                        fheld[c, h] = totals[1 - axis][at]
                        if direct_rs(c):
                            fsend[c, 2, h] = totals[1 - axis][at].astype(BF16)

            @pl.when(even)
            def _():
                if direct_rs(c):
                    far_direct(c).start()
                for kind in range(1 if direct_rs(c) else 0, 3 if direct_rs(c) else 2):
                    for h in range(halves):
                        far_copy(c, h, kind).start()

        else:
            for i in order:
                fsend[c, i, 0] = toward(i).astype(BF16)
                far_copy(c, 0, i).start()

    for loads in late:
        start_load(loads)
    with scope("enwait"):
        live_load[1].wait()
        near_load[1].wait()
    for k in range(3):
        for t in range(tiles):
            flag = live[0, k, t].astype(F32).astype(BF16)
            at = pl.ds(t * rows, rows)
            inc[long_count + k, :, at] = inc[long_count + k, :, at] * flag
    for c in range(CHUNKS):
        cols = pl.ds(c * width, width)
        near_all = mm(inc[pl.ds(long_count, 3)].reshape(3 * rows, gs.shape[0]), em[c])
        for s, k in ((0, 0), (1, 2)):
            nsend[s, c] = near_all[k * rows:(k + 1) * rows].astype(BF16)
        start_side(near_copy, c)
        own_near[:, cols] = near_all[rows:2 * rows].astype(BF16)

    if relay:
        @pl.when(even)
        def _():
            with scope("rsdrain"):
                whole(fsend.at[0], fs_sem.at[0], fs_sem.at[0]).wait_send()
            hand_over(0)

        @pl.when(odd)
        def _():
            with scope("rsturn"):
                pl.semaphore_wait(turn.at[0], 1)
            for kind in range(2):
                for c in range(CHUNKS):
                    for h in range(halves):
                        far_copy(c, h, kind).start()

        def pass_on(c):
            for h in range(halves):
                with scope("relaywait"):
                    far_copy(c, h, 0).wait_recv()
                fsend[c, 2, h] = (fheld[c, h] + frelay[c, h].astype(F32)).astype(BF16)
                far_copy(c, h, 2).start()

        for c in range(CHUNKS):
            if direct_rs(c):
                @pl.when(odd)
                def _():
                    pass_on(c)
            else:
                pass_on(c)

    for loads in late:
        loads[1].wait()
    for i in range(far_count):
        total = None
        for index in range(long_count):
            flag = jnp.where(regions[1, 0, index] == peers[i][1], 1.0, 0.0).astype(F32)
            term = pinc[3 + index].astype(F32) * flag
            total = term if total is None else total + term
        proc_inc[i] = total.astype(BF16)
    for k in range(3):
        for t in range(tiles):
            at = pl.ds(t * rows, rows)
            dn[k, at, :] = dn[k, at, :] * live[1, k, t].astype(F32).astype(BF16)

    def node_update(residual, summed, first, second):
        hidden = silu(mm(layer_norm(summed).astype(BF16), wt[first])).astype(BF16)
        return (residual.astype(F32) + mm(hidden, wt[second])).astype(BF16)

    with scope("nearwait"):
        for s in range(2):
            wait_side(nrecv, nr_sem, s)
    parts = []
    for c in range(CHUNKS):
        total = own_near[:, pl.ds(c * width, width)].astype(F32)
        for s in range(2):
            total = total + nrecv[s, c].astype(F32)
        slots = 3 if direct_rs(c) else 2 if relay else far_count
        with scope("farwait"):
            if direct_rs(c):
                @pl.when(even)
                def _():
                    whole(frecv.at[c], fr_sem.at[c], fr_sem.at[c]).wait_recv()

                @pl.when(odd)
                def _():
                    whole(frecv.at[c, pl.ds(0, 2)], fr_sem.at[c], fr_sem.at[c]).wait_recv()
            else:
                whole(frecv.at[c, pl.ds(0, slots)], fr_sem.at[c], fr_sem.at[c]).wait_recv()
        pieces = []
        for h in range(halves):
            piece = total[h * piece_rows:(h + 1) * piece_rows]
            for i in range(slots):
                piece = piece + frecv[c, i, h].astype(F32)
            pieces.append(piece)
        parts.append(jnp.concatenate(pieces, axis=0))
    with scope("upd1"):
        mesh_mid = node_update(ms[...], jnp.concatenate(parts, axis=1), 1, 2)

    for c in range(CHUNKS):
        msend[c] = silu(mm(mesh_mid, wt[3, :, pl.ds(c * width, width)])).astype(BF16)
        if not relay:
            for i in order:
                mfar_copy(c, 0, i).start()
        else:
            @pl.when(even)
            def _():
                if direct_ag(c):
                    mfar_direct(c).start()
                for h in range(halves):
                    mfar_copy(c, h, first_axis(h)).start()
                    mfar_copy(c, h, 1 - first_axis(h)).start()
        start_side(mnear_copy, c)

    def send_second():
        for c in range(CHUNKS):
            for h in range(halves):
                mfar_copy(c, h, 1 - first_axis(h)).start()

    if relay:
        @pl.when(odd)
        def _():
            with scope("oddwait"):
                pl.semaphore_wait(turn.at[1], 1)
            for c in range(CHUNKS):
                for h in range(halves):
                    mfar_copy(c, h, first_axis(h)).start()
            send_second()
    parts = [mm(pinc[1], msend[c]) for c in range(CHUNKS)]
    if relay:
        @pl.when(even)
        def _():
            with scope("agdrain"):
                whole(mfrecv.at[0], mfs_sem.at[0], mfs_sem.at[0]).wait_send()
            hand_over(1)
    if relay:
        for c in range(CHUNKS):
            for h in range(halves):
                with scope("mrelaywait"):
                    mfar_copy(c, h, first_axis(h)).wait_recv()
                if direct_ag(c):
                    @pl.when(odd)
                    def _():
                        mfar_copy(c, h, 2).start()
                else:
                    mfar_copy(c, h, 2).start()
    for s in range(2):
        with scope("mnearwait"):
            wait_side(mnrecv, mnr_sem, s)
        for c in range(CHUNKS):
            parts[c] = parts[c] + mm(pinc[2 * s], mnrecv[s, c])
    for c in range(CHUNKS):
        with scope("mfarwait"):
            if relay:
                whole(mfrecv.at[c, 0], mfr_sem.at[c, 0], mfr_sem.at[c, 0]).wait_recv()
            else:
                whole(mfrecv.at[c], mfr_sem.at[c, 0], mfr_sem.at[c, 0]).wait_recv()
        for i in range(2 if relay else far_count):
            parts[c] = parts[c] + mm(proc_inc[i], mfrecv[c, i])
    if relay:
        for c in range(CHUNKS):
            with scope("mdiagwait"):
                whole(mfrecv.at[c, 2], mfr_sem.at[c, 1], mfr_sem.at[c, 1]).wait_recv()
            parts[c] = parts[c] + mm(proc_inc[2], mfrecv[c, 2])
    with scope("upd2"):
        mesh_next = node_update(mesh_mid, jnp.concatenate(parts, axis=1), 4, 5)
    mesh_out[...] = mesh_next

    for c in range(CHUNKS):
        dsend[c] = silu(mm(mesh_next, wt[6, :, pl.ds(c * width, width)])).astype(BF16)
        start_side(dec_copy, c)

    block = 2 * rows

    def decode(add, c, k, source):
        for i in range(gs.shape[0] // block):
            at = pl.ds(i * block, block)
            part = mm(dn[k, at, :], source)
            acc[at, pl.ds(c * width, width)] = acc[at, pl.ds(c * width, width)] + part if add else part

    with scope("ownpart"):
        for c in range(CHUNKS):
            decode(False, c, 1, dsend[c])
    for s in (near_side, 1 - near_side):
        there = jnp.where(s == 0, not_first, not_last)
        for c in range(CHUNKS):
            with scope("decwait"):
                @pl.when(there)
                def _():
                    whole(dnrecv.at[s, c], dr_sem.at[s, c], dr_sem.at[s, c]).wait_recv()
            decode(True, c, 2 * s, dnrecv[s, c])

    with scope("drain"):
        def far_sent(c):
            whole(fsend.at[c], fs_sem.at[c], fs_sem.at[c]).wait_send()
            whole(mfrecv.at[c], mfs_sem.at[c], mfs_sem.at[c]).wait_send()

        for c in range(CHUNKS):
            if relay and c == 0:
                pl.when(odd)(functools.partial(far_sent, c))
            else:
                far_sent(c)
        for s, (there, _) in enumerate(sides):
            @pl.when(there)
            def _():
                whole(nsend.at[s], ns_sem.at[s], ns_sem.at[s]).wait_send()
                whole(msend, mns_sem.at[s], mns_sem.at[s]).wait_send()
                whole(dsend, ds_sem.at[s], ds_sem.at[s]).wait_send()


def finish(mesh_v, gs, dw, acc, grid_o, mesh_o, grid_out, out_sem):
    step = gs.shape[0] // (out_sem.shape[0] - 1)
    width = gs.shape[1] // CHUNKS
    mesh_copy = pltpu.make_async_copy(mesh_v, mesh_o, out_sem.at[0])
    mesh_copy.start()
    outs = []
    for i in range(gs.shape[0] // step):
        at = pl.ds(i * step, step)
        normed = layer_norm(acc[at, :]).astype(BF16)
        parts = [silu(mm(normed, dw[0, :, pl.ds(c * width, width)])).astype(BF16) for c in range(CHUNKS)]
        hidden = jnp.concatenate(parts, axis=1)
        for c in range(CHUNKS):
            cols = pl.ds(c * width, width)
            grid_out[at, cols] = (gs[at, cols].astype(F32) + mm(hidden, dw[1, :, cols])).astype(BF16)
        copy = pltpu.make_async_copy(grid_out.at[at], grid_o.at[at], out_sem.at[1 + i])
        copy.start()
        outs.append(copy)
    with scope("outwait"):
        mesh_copy.wait()
        for copy in outs:
            copy.wait()


def body(groups, devs, *args):
    grid_state, mesh_state = args[0], args[1]
    args = list(args)
    args[14], args[17] = args[14].T, args[17].T
    encode_live, encode_far, encode_groups, decode_near = args[12], args[13], args[14], args[18]
    grid_rows, feats = grid_state.shape
    rows = mesh_state.shape[0]
    width = feats // CHUNKS
    far_count = groups - 1
    long_count = encode_far.shape[0]

    def vmem(*shape, dtype=BF16):
        return pltpu.VMEM(shape, dtype)

    dma = pltpu.SemaphoreType.DMA
    relay = groups == 4
    halves = 2 if relay else 1
    piece = (rows // halves, width)
    block = (rows, width)
    scratch = [
        vmem(rows, feats), vmem(7, feats, feats), vmem(3 + long_count, rows, grid_rows),
        pltpu.SMEM((2, *encode_live.shape), jnp.int32), pltpu.SMEM((2, *encode_groups.shape), jnp.int32),
        vmem(3 + long_count, rows, rows), vmem(*decode_near.shape),
        vmem(CHUNKS, grid_rows, width),
        vmem(CHUNKS, halves, *piece, dtype=F32), vmem(CHUNKS, far_count, halves, *piece),
        vmem(CHUNKS, halves, *piece), vmem(CHUNKS, far_count, halves, *piece),
        vmem(2, CHUNKS, *block), vmem(2, CHUNKS, *block),
        vmem(CHUNKS, *block), vmem(CHUNKS, far_count, *block), vmem(2, CHUNKS, *block),
        vmem(CHUNKS, *block), vmem(2, CHUNKS, *block),
        vmem(rows, feats), vmem(far_count, rows, rows),
        dma((11,)), dma((GRID_LOADS,)), dma((CHUNKS,)), dma((CHUNKS, halves)), dma((CHUNKS,)), dma((2,)), dma((2,)),
        dma((CHUNKS,)), dma((CHUNKS, halves)), dma((CHUNKS, halves)), dma((2,)), dma((2,)), dma((2,)), dma((2, CHUNKS)), pltpu.SemaphoreType.REGULAR((2,)),
    ]
    hbm = pl.BlockSpec(memory_space=pltpu.HBM)
    on_chip = pl.BlockSpec(memory_space=pltpu.VMEM)
    held = pl.pallas_call(
        functools.partial(exchange, groups, devs),
        out_shape=(
            vmem(*mesh_state.shape), vmem(*grid_state.shape), vmem(2, feats, feats), vmem(*grid_state.shape, dtype=F32),
        ),
        in_specs=[hbm] * len(args),
        out_specs=(on_chip,) * 4,
        scratch_shapes=scratch,
        compiler_params=pltpu.CompilerParams(collective_id=0, has_side_effects=True, vmem_limit_bytes=32 << 20),
        name="exchange",
    )(*(pltpu.with_memory_space_constraint(arg, pltpu.HBM) for arg in args))
    return pl.pallas_call(
        finish,
        out_shape=(
            jax.ShapeDtypeStruct(grid_state.shape, BF16),
            jax.ShapeDtypeStruct(mesh_state.shape, BF16),
        ),
        in_specs=[on_chip] * 4,
        out_specs=(hbm, hbm),
        scratch_shapes=[vmem(*grid_state.shape), dma((1 + GRID_OUTS,))],
        compiler_params=pltpu.CompilerParams(vmem_limit_bytes=16 << 20),
        name="finish",
    )(*held)


def solution(mesh):
    both = ("group", "dev")
    row, whole, second = P(both, None), P(), P(None, both, None)
    flags = P(None, both)
    return jax.shard_map(
        functools.partial(body, mesh.shape["group"], mesh.shape["dev"]),
        mesh=mesh,
        in_specs=(
            row, row, whole, whole, whole, whole, whole, whole, whole, whole, whole,
            second, flags, second, flags, second, second, flags, second, flags,
        ),
        out_specs=(row, row),
        check_vma=False,
    )
```

```python
import contextlib
import functools

import jax
import jax.numpy as jnp
from jax import lax
from jax.experimental import pallas as pl
from jax.experimental.pallas import tpu as pltpu
from jax.sharding import PartitionSpec as P

BF16 = jnp.bfloat16
F32 = jnp.float32
CHUNKS = 2
GRID_CUT = 4
GRID_OUTS = 2
ODD_RS = 1
ODD_AG = 1


def gate(half):
    return half + half * jnp.tanh(half)


def silu(x):
    return gate(0.5 * x)


def mm(a, b):
    return jnp.dot(a, b, preferred_element_type=F32)


def centred(v):
    cent = v - jnp.mean(v, axis=-1, keepdims=True)
    var = jnp.mean(cent * cent, axis=-1, keepdims=True)
    return cent.astype(BF16), 0.5 * lax.rsqrt(var + 1e-05)


def partner(me, r, count):
    if count & (count - 1):
        return lax.rem(me + r, count), lax.rem(me + count - r, count)
    out, bit = me, 1
    while bit < count:
        if r & bit:
            out = out + bit * (1 - 2 * lax.rem(me // bit, 2))
        bit *= 2
    return out, out


def scope(name):
    return contextlib.nullcontext()


def exchange(
    groups,
    devs,
    grid_h, mesh_h, ee_h, e1_h, e2_h, pe_h, p1_h, p2_h, de_h, d1_h, d2_h,
    en_h, el_h, ef_h, eg_h, pn_h, pf_h, pg_h, dn_h, dl_h,
    mesh_out, gs, dw, acc, dn, last,
    ms, wt, inc, live, regions, pinc,
    em, fheld, fsend, frelay, frecv, nsend, nrecv, msend, mfrecv, mnrecv, dsend, dnrecv,
    own_near, proc_inc,
    load_sem, grid_sem, fs_sem, fl_sem, fr_sem, ns_sem, nr_sem, mfs_sem, mfl_sem, mfr_sem, mns_sem, mnr_sem, ds_sem, dr_sem, turn,
):
    g = lax.axis_index("group")
    d = lax.axis_index("dev")
    rows, feats = ms.shape
    width = feats // CHUNKS
    far_count = groups - 1
    long_count = pinc.shape[0] - 3
    tiles = live.shape[2]
    peers = [partner(g, r, groups) for r in range(1, groups)]
    order = list(reversed(range(far_count)))
    relay = groups == 4
    halves = fsend.shape[2]
    piece_rows = rows // halves
    if groups & (groups - 1):
        greeted = [to for to, _ in peers] + [source for _, source in peers]
    else:
        greeted = [to for to, _ in peers]
    not_first, not_last = d > 0, d < devs - 1
    sides = ((not_first, d - 1), (not_last, d + 1))
    far_side = lax.rem(d, 2)
    near_side = 1 - far_side
    even, odd = lax.rem(d, 2) == 0, lax.rem(d, 2) == 1

    def load(index, pairs, whole):
        starts = [pltpu.make_async_copy(src, dst, load_sem.at[index]) for src, dst in pairs]
        return starts, pltpu.make_async_copy(whole, whole, load_sem.at[index])

    far_inc, near_inc = inc.at[pl.ds(0, long_count)], inc.at[pl.ds(long_count, 3)]
    first = load(0, [(ee_h, wt.at[0])], wt.at[0])
    far_load = load(1, [(ef_h, far_inc)], far_inc)
    near_load = load(2, [(en_h, near_inc)], near_inc)
    live_load = load(3, [(el_h, live.at[0]), (dl_h, live.at[1])], live)
    region_load = load(4, [(eg_h, regions.at[0]), (pg_h, regions.at[1])], regions)
    late = [
        load(5, [(mesh_h, ms)], ms),
        load(6, [(h, wt.at[1 + i]) for i, h in enumerate((e1_h, e2_h, pe_h, p1_h, p2_h, de_h))], wt.at[pl.ds(1, 6)]),
        load(7, [(pn_h, pinc.at[pl.ds(0, 3)]), (pf_h, pinc.at[pl.ds(3, long_count)])], pinc),
        load(8, [(dn_h, dn)], dn),
        load(9, [(d1_h, dw.at[0]), (d2_h, dw.at[1])], dw),
    ]

    def start_load(loads):
        for copy in loads[0]:
            copy.start()

    cut = gs.shape[0] // GRID_CUT
    grid_rows = [pl.ds(0, cut), pl.ds(cut, gs.shape[0] - cut)]
    count = len(grid_rows)
    grid_loads = [pltpu.make_async_copy(grid_h.at[at], gs.at[at], grid_sem.at[i]) for i, at in enumerate(grid_rows)]
    start_load(first)
    for copy in grid_loads:
        copy.start()
    for loads in (region_load, far_load, live_load, near_load):
        start_load(loads)

    barrier = pltpu.get_barrier_semaphore()
    for to in greeted:
        pl.semaphore_signal(barrier, inc=1, device_id=(to, d), device_id_type=pl.DeviceIdType.MESH)
    for there, near in sides:
        @pl.when(there)
        def _():
            pl.semaphore_signal(barrier, inc=1, device_id=(g, near), device_id_type=pl.DeviceIdType.MESH)

    for side, (there, _) in enumerate(sides):
        @pl.when(jnp.logical_not(there))
        def _():
            for buf in (nrecv, mnrecv, dnrecv):
                for c in range(CHUNKS):
                    buf[side, c] = jnp.zeros((rows, width), BF16)

    if relay:
        @pl.when(odd)
        def _():
            for c in range(ODD_RS):
                frecv[c, 2] = jnp.zeros(frecv.shape[2:], BF16)

    def remote(src, dst, send, recv, to):
        return pltpu.make_async_remote_copy(
            src_ref=src, dst_ref=dst, send_sem=send, recv_sem=recv, device_id=to, device_id_type=pl.DeviceIdType.MESH
        )

    def whole(ref, send, recv):
        return remote(ref, ref, send, recv, (peers[0][0], d))

    def hand_over(phase):
        @pl.when(not_last)
        def _():
            pl.semaphore_signal(turn.at[phase], inc=1, device_id=(g, d + 1), device_id_type=pl.DeviceIdType.MESH)

    def first_axis(h):
        return h % 2

    def far_copy(c, h, kind):
        if not relay:
            return remote(fsend.at[c, kind, h], frecv.at[c, kind, h], fs_sem.at[c], fr_sem.at[c], (peers[kind][0], d))
        to = first_axis(h) if kind < 2 else 1 - first_axis(h)
        if kind == 0:
            return remote(fsend.at[c, 0, h], frelay.at[c, h], fs_sem.at[c], fl_sem.at[c, h], (peers[to][0], d))
        return remote(fsend.at[c, kind, h], frecv.at[c, kind - 1, h], fs_sem.at[c], fr_sem.at[c], (peers[to][0], d))

    def far_direct(c):
        return remote(fsend.at[c, 0], frecv.at[c, 2], fs_sem.at[c], fr_sem.at[c], (peers[2][0], d))

    def mfar_direct(c):
        return remote(msend.at[c], mfrecv.at[c, 2], mfs_sem.at[c], mfr_sem.at[c, 1], (peers[2][0], d))

    def near_copy(c, s):
        return remote(nsend.at[s, c], nrecv.at[1 - s, c], ns_sem.at[s], nr_sem.at[1 - s], (g, sides[s][1]))

    def mfar_copy(c, h, i):
        at = pl.ds(h * piece_rows, piece_rows)
        source, to, recv = msend.at[c, at], i, mfr_sem.at[c, 0]
        if relay:
            if i == 2:
                source, to, recv = mfrecv.at[c, first_axis(h), at], 1 - first_axis(h), mfr_sem.at[c, 1]
            elif i == first_axis(h) and c < ODD_AG:
                recv = mfl_sem.at[c, h]
        return remote(source, mfrecv.at[c, i, at], mfs_sem.at[c], recv, (peers[to][0], d))

    def mnear_copy(c, s):
        return remote(msend.at[c], mnrecv.at[1 - s, c], mns_sem.at[s], mnr_sem.at[1 - s], (g, sides[s][1]))

    def dec_copy(c, s):
        return remote(dsend.at[c], dnrecv.at[1 - s, c], ds_sem.at[s], dr_sem.at[1 - s, c], (g, sides[s][1]))

    def start_side(copy, c):
        for s, (there, _) in enumerate(sides):
            @pl.when(there)
            def _():
                copy(c, s).start()

    def wait_side(buf, sem, s):
        @pl.when(sides[s][0])
        def _():
            whole(buf.at[s], sem.at[s], sem.at[s]).wait_recv()

    greetings = len(greeted) + jnp.where(not_first, 1, 0) + jnp.where(not_last, 1, 0)
    with scope("ldwait"):
        first[1].wait()
    for c in range(CHUNKS):
        cols = pl.ds(c * width, width)
        for i in range(count):
            if c == 0:
                with scope("gridwait"):
                    grid_loads[i].wait()
                    if i == count - 1:
                        region_load[1].wait()
                        far_load[1].wait()
                        pl.semaphore_wait(barrier, greetings)
            at = grid_rows[i]
            em[c, at, :] = silu(mm(gs[at, :], wt[0, :, cols])).astype(BF16)
        far_all = mm(inc[pl.ds(0, long_count)].reshape(long_count * rows, gs.shape[0]), em[c])
        far = [far_all[i * rows:(i + 1) * rows] for i in range(long_count)]

        def toward(i):
            total = None
            for index in range(long_count):
                flag = jnp.where(regions[0, 0, index] == peers[i][0], 1.0, 0.0).astype(F32)
                term = far[index] * flag
                total = term if total is None else total + term
            return total

        if relay:
            totals = [toward(i) for i in range(far_count)]
            for kind in range(2):
                for h in range(halves):
                    at = slice(h * piece_rows, (h + 1) * piece_rows)
                    axis = first_axis(h)
                    fsend[c, kind, h] = totals[2 if kind == 0 else axis][at].astype(BF16)
                    if kind == 0:
                        fheld[c, h] = totals[1 - axis][at]
                        if True:
                            fsend[c, 2, h] = totals[1 - axis][at].astype(BF16)

            @pl.when(even)
            def _():
                far_direct(c).start()
                for kind in (1, 2):
                    for h in range(halves):
                        far_copy(c, h, kind).start()

        else:
            for i in order:
                fsend[c, i, 0] = toward(i).astype(BF16)
                far_copy(c, 0, i).start()

    for loads in late:
        start_load(loads)
    with scope("enwait"):
        live_load[1].wait()
        near_load[1].wait()
    for k in range(3):
        for t in range(tiles):
            flag = live[0, k, t].astype(F32).astype(BF16)
            at = pl.ds(t * rows, rows)
            inc[long_count + k, :, at] = inc[long_count + k, :, at] * flag
    for c in range(CHUNKS):
        cols = pl.ds(c * width, width)
        near_all = mm(inc[pl.ds(long_count, 3)].reshape(3 * rows, gs.shape[0]), em[c])
        for s, k in ((0, 0), (1, 2)):
            nsend[s, c] = near_all[k * rows:(k + 1) * rows].astype(BF16)
        start_side(near_copy, c)
        own_near[:, cols] = near_all[rows:2 * rows].astype(BF16)

    if relay:
        @pl.when(even)
        def _():
            with scope("rsdrain"):
                whole(fsend.at[0], fs_sem.at[0], fs_sem.at[0]).wait_send()
            hand_over(0)

        @pl.when(odd)
        def _():
            with scope("rsturn"):
                pl.semaphore_wait(turn.at[0], 1)
            for c in range(ODD_RS):
                for h in range(halves):
                    far_copy(c, h, 0).start()
            for c in range(ODD_RS, CHUNKS):
                far_direct(c).start()
            for c in range(CHUNKS):
                for kind in (1, 2) if c >= ODD_RS else (1,):
                    for h in range(halves):
                        far_copy(c, h, kind).start()

        def pass_on(c):
            for h in range(halves):
                with scope("relaywait"):
                    far_copy(c, h, 0).wait_recv()
                fsend[c, 2, h] = (fheld[c, h] + frelay[c, h].astype(F32)).astype(BF16)
                far_copy(c, h, 2).start()

        for c in range(ODD_RS):
            pl.when(odd)(functools.partial(pass_on, c))

    for loads in late:
        loads[1].wait()
    for i in range(far_count):
        total = None
        for index in range(long_count):
            flag = jnp.where(regions[1, 0, index] == peers[i][1], 1.0, 0.0).astype(F32)
            term = pinc[3 + index].astype(F32) * flag
            total = term if total is None else total + term
        proc_inc[i] = total.astype(BF16)
    for k in range(3):
        for t in range(tiles):
            at = pl.ds(t * rows, rows)
            dn[k, at, :] = dn[k, at, :] * live[1, k, t].astype(F32).astype(BF16)

    def node_update(residual, summed, first, second):
        cent, half = centred(summed)
        hidden = gate(half * mm(cent, wt[first])).astype(BF16)
        return (residual.astype(F32) + mm(hidden, wt[second])).astype(BF16)

    with scope("nearwait"):
        for s in range(2):
            wait_side(nrecv, nr_sem, s)
    parts = []
    for c in range(CHUNKS):
        total = own_near[:, pl.ds(c * width, width)].astype(F32)
        for s in range(2):
            total = total + nrecv[s, c].astype(F32)
        slots = far_count
        with scope("farwait"):
            if relay and c < ODD_RS:
                @pl.when(even)
                def _():
                    whole(frecv.at[c], fr_sem.at[c], fr_sem.at[c]).wait_recv()

                @pl.when(odd)
                def _():
                    whole(frecv.at[c, pl.ds(0, 2)], fr_sem.at[c], fr_sem.at[c]).wait_recv()
            else:
                whole(frecv.at[c, pl.ds(0, slots)], fr_sem.at[c], fr_sem.at[c]).wait_recv()
        pieces = []
        for h in range(halves):
            piece = total[h * piece_rows:(h + 1) * piece_rows]
            for i in range(slots):
                piece = piece + frecv[c, i, h].astype(F32)
            pieces.append(piece)
        parts.append(jnp.concatenate(pieces, axis=0))
    with scope("upd1"):
        mesh_mid = node_update(ms[...], jnp.concatenate(parts, axis=1), 1, 2)

    for c in range(CHUNKS):
        msend[c] = silu(mm(mesh_mid, wt[3, :, pl.ds(c * width, width)])).astype(BF16)
        if not relay:
            for i in order:
                mfar_copy(c, 0, i).start()
        else:
            @pl.when(even)
            def _():
                mfar_direct(c).start()
                for h in range(halves):
                    mfar_copy(c, h, first_axis(h)).start()
                    mfar_copy(c, h, 1 - first_axis(h)).start()
        start_side(mnear_copy, c)

    def send_second():
        for c in range(CHUNKS):
            for h in range(halves):
                mfar_copy(c, h, 1 - first_axis(h)).start()

    if relay:
        @pl.when(odd)
        def _():
            with scope("oddwait"):
                pl.semaphore_wait(turn.at[1], 1)
            for c in range(CHUNKS):
                for h in range(halves):
                    mfar_copy(c, h, first_axis(h)).start()
            for c in range(ODD_AG, CHUNKS):
                mfar_direct(c).start()
            send_second()
    parts = [mm(pinc[1], msend[c]) for c in range(CHUNKS)]
    if relay:
        @pl.when(even)
        def _():
            with scope("agdrain"):
                whole(mfrecv.at[0], mfs_sem.at[0], mfs_sem.at[0]).wait_send()
            hand_over(1)
    if relay:
        for c in range(ODD_AG):
            for h in range(halves):
                with scope("mrelaywait"):
                    mfar_copy(c, h, first_axis(h)).wait_recv()

                @pl.when(odd)
                def _():
                    mfar_copy(c, h, 2).start()
    for s in range(2):
        with scope("mnearwait"):
            wait_side(mnrecv, mnr_sem, s)
        for c in range(CHUNKS):
            parts[c] = parts[c] + mm(pinc[2 * s], mnrecv[s, c])
    for c in range(CHUNKS):
        with scope("mfarwait"):
            if relay:
                own = mfrecv.at[c, 0] if c < ODD_AG else mfrecv.at[c, pl.ds(0, 2)]
                whole(own, mfr_sem.at[c, 0], mfr_sem.at[c, 0]).wait_recv()
            else:
                whole(mfrecv.at[c], mfr_sem.at[c, 0], mfr_sem.at[c, 0]).wait_recv()
        for i in range(2 if relay else far_count):
            parts[c] = parts[c] + mm(proc_inc[i], mfrecv[c, i])
    if relay:
        for c in range(CHUNKS):
            with scope("mdiagwait"):
                whole(mfrecv.at[c, 2], mfr_sem.at[c, 1], mfr_sem.at[c, 1]).wait_recv()
            parts[c] = parts[c] + mm(proc_inc[2], mfrecv[c, 2])
    with scope("upd2"):
        mesh_next = node_update(mesh_mid, jnp.concatenate(parts, axis=1), 4, 5)
    mesh_out[...] = mesh_next

    for c in range(CHUNKS):
        dsend[c] = silu(mm(mesh_next, wt[6, :, pl.ds(c * width, width)])).astype(BF16)
        start_side(dec_copy, c)

    block = 2 * rows

    def decode(add, c, k, source):
        for i in range(gs.shape[0] // block):
            at = pl.ds(i * block, block)
            part = mm(dn[k, at, :], source)
            acc[at, pl.ds(c * width, width)] = acc[at, pl.ds(c * width, width)] + part if add else part

    with scope("ownpart"):
        for c in range(CHUNKS):
            decode(False, c, 1, dsend[c])
    for s in (near_side, far_side):
        there = jnp.where(s == 0, not_first, not_last)
        for c in range(CHUNKS):
            with scope("decwait"):
                @pl.when(there)
                def _():
                    whole(dnrecv.at[s, c], dr_sem.at[s, c], dr_sem.at[s, c]).wait_recv()
            if s is near_side or c < CHUNKS - 1:
                decode(True, c, 2 * s, dnrecv[s, c])
    last[...] = dnrecv[far_side, CHUNKS - 1]

    with scope("drain"):
        def far_sent(c):
            whole(fsend.at[c], fs_sem.at[c], fs_sem.at[c]).wait_send()
            whole(mfrecv.at[c], mfs_sem.at[c], mfs_sem.at[c]).wait_send()

        for c in range(CHUNKS):
            if relay and c == 0:
                pl.when(odd)(functools.partial(far_sent, c))
            else:
                far_sent(c)
        for s, (there, _) in enumerate(sides):
            @pl.when(there)
            def _():
                whole(nsend.at[s], ns_sem.at[s], ns_sem.at[s]).wait_send()
                whole(msend, mns_sem.at[s], mns_sem.at[s]).wait_send()
                whole(dsend, ds_sem.at[s], ds_sem.at[s]).wait_send()


def finish(mesh_v, gs, dw, acc, dn, last, grid_o, mesh_o, grid_out, out_sem):
    step = gs.shape[0] // (out_sem.shape[0] - 1)
    width = gs.shape[1] // CHUNKS
    side = lax.rem(lax.axis_index("dev"), 2)
    mesh_copy = pltpu.make_async_copy(mesh_v, mesh_o, out_sem.at[0])
    mesh_copy.start()
    outs = []
    for i in range(gs.shape[0] // step):
        at = pl.ds(i * step, step)
        held = [acc[at, pl.ds(c * width, width)] for c in range(CHUNKS)]
        held[-1] = held[-1] + mm(dn[2 * side, at, :], last[...])
        cent, half = centred(jnp.concatenate(held, axis=1))
        parts = [gate(half * mm(cent, dw[0, :, pl.ds(c * width, width)])).astype(BF16) for c in range(CHUNKS)]
        hidden = jnp.concatenate(parts, axis=1)
        for c in range(CHUNKS):
            cols = pl.ds(c * width, width)
            grid_out[at, cols] = (gs[at, cols].astype(F32) + mm(hidden, dw[1, :, cols])).astype(BF16)
        copy = pltpu.make_async_copy(grid_out.at[at], grid_o.at[at], out_sem.at[1 + i])
        copy.start()
        outs.append(copy)
    with scope("outwait"):
        mesh_copy.wait()
        for copy in outs:
            copy.wait()


def body(groups, devs, *args):
    grid_state, mesh_state = args[0], args[1]
    args = list(args)
    args[14], args[17] = args[14].T, args[17].T
    encode_live, encode_far, encode_groups, decode_near = args[12], args[13], args[14], args[18]
    grid_rows, feats = grid_state.shape
    rows = mesh_state.shape[0]
    width = feats // CHUNKS
    far_count = groups - 1
    long_count = encode_far.shape[0]

    def vmem(*shape, dtype=BF16):
        return pltpu.VMEM(shape, dtype)

    dma = pltpu.SemaphoreType.DMA
    relay = groups == 4
    halves = 2 if relay else 1
    piece = (rows // halves, width)
    block = (rows, width)
    scratch = [
        vmem(rows, feats), vmem(7, feats, feats), vmem(3 + long_count, rows, grid_rows),
        pltpu.SMEM((2, *encode_live.shape), jnp.int32), pltpu.SMEM((2, *encode_groups.shape), jnp.int32),
        vmem(3 + long_count, rows, rows),
        vmem(CHUNKS, grid_rows, width),
        vmem(CHUNKS, halves, *piece, dtype=F32), vmem(CHUNKS, far_count, halves, *piece),
        vmem(CHUNKS, halves, *piece), vmem(CHUNKS, far_count, halves, *piece),
        vmem(2, CHUNKS, *block), vmem(2, CHUNKS, *block),
        vmem(CHUNKS, *block), vmem(CHUNKS, far_count, *block), vmem(2, CHUNKS, *block),
        vmem(CHUNKS, *block), vmem(2, CHUNKS, *block),
        vmem(rows, feats), vmem(far_count, rows, rows),
        dma((10,)), dma((2,)), dma((CHUNKS,)), dma((ODD_RS, halves)), dma((CHUNKS,)), dma((2,)), dma((2,)),
        dma((CHUNKS,)), dma((ODD_AG, halves)), dma((CHUNKS, 2)), dma((2,)), dma((2,)), dma((2,)), dma((2, CHUNKS)), pltpu.SemaphoreType.REGULAR((2,)),
    ]
    hbm = pl.BlockSpec(memory_space=pltpu.HBM)
    on_chip = pl.BlockSpec(memory_space=pltpu.VMEM)
    held = pl.pallas_call(
        functools.partial(exchange, groups, devs),
        out_shape=(
            vmem(*mesh_state.shape), vmem(*grid_state.shape), vmem(2, feats, feats), vmem(*grid_state.shape, dtype=F32),
            vmem(*decode_near.shape), vmem(*block),
        ),
        in_specs=[hbm] * len(args),
        out_specs=(on_chip,) * 6,
        scratch_shapes=scratch,
        compiler_params=pltpu.CompilerParams(collective_id=0, has_side_effects=True, vmem_limit_bytes=32 << 20),
        name="exchange",
    )(*(pltpu.with_memory_space_constraint(arg, pltpu.HBM) for arg in args))
    return pl.pallas_call(
        finish,
        out_shape=(
            jax.ShapeDtypeStruct(grid_state.shape, BF16),
            jax.ShapeDtypeStruct(mesh_state.shape, BF16),
        ),
        in_specs=[on_chip] * 6,
        out_specs=(hbm, hbm),
        scratch_shapes=[vmem(*grid_state.shape), dma((1 + GRID_OUTS,))],
        compiler_params=pltpu.CompilerParams(vmem_limit_bytes=16 << 20),
        name="finish",
    )(*held)


def solution(mesh):
    both = ("group", "dev")
    row, whole, second = P(both, None), P(), P(None, both, None)
    flags = P(None, both)
    return jax.shard_map(
        functools.partial(body, mesh.shape["group"], mesh.shape["dev"]),
        mesh=mesh,
        in_specs=(
            row, row, whole, whole, whole, whole, whole, whole, whole, whole, whole,
            second, flags, second, flags, second, second, flags, second, flags,
        ),
        out_specs=(row, row),
        check_vma=False,
    )
```

```python
import contextlib
import functools

import jax
import jax.numpy as jnp
from jax import lax
from jax.experimental import pallas as pl
from jax.experimental.pallas import tpu as pltpu
from jax.sharding import PartitionSpec as P

BF16 = jnp.bfloat16
F32 = jnp.float32
CHUNKS = 2
GRID_CUT = 4
GRID_OUTS = 2
ODD_RS = 1
ODD_AG = 1


def gate(half):
    return half + half * jnp.tanh(half)


def silu(x):
    return gate(0.5 * x)


def mm(a, b):
    return jnp.dot(a, b, preferred_element_type=F32)


def centred(v):
    cent = v - jnp.mean(v, axis=-1, keepdims=True)
    var = jnp.mean(cent * cent, axis=-1, keepdims=True)
    return cent.astype(BF16), 0.5 * lax.rsqrt(var + 1e-05)


def partner(me, r, count):
    if count & (count - 1):
        return lax.rem(me + r, count), lax.rem(me + count - r, count)
    out, bit = me, 1
    while bit < count:
        if r & bit:
            out = out + bit * (1 - 2 * lax.rem(me // bit, 2))
        bit *= 2
    return out, out


def scope(name):
    return contextlib.nullcontext()


def exchange(
    groups,
    devs,
    grid_h, mesh_h, ee_h, e1_h, e2_h, pe_h, p1_h, p2_h, de_h, d1_h, d2_h,
    en_h, el_h, ef_h, eg_h, pn_h, pf_h, pg_h, dn_h, dl_h,
    mesh_out, gs, dw, acc, dn, last,
    ms, wt, inc, live, regions, pinc,
    em, fheld, fsend, frelay, frecv, nsend, nrecv, msend, mfrecv, mnrecv, dsend, dnrecv,
    own_near, proc_inc,
    load_sem, grid_sem, fs_sem, fl_sem, fr_sem, ns_sem, nr_sem, mfs_sem, mfl_sem, mfr_sem, mns_sem, mnr_sem, ds_sem, dr_sem, turn,
):
    g = lax.axis_index("group")
    d = lax.axis_index("dev")
    rows, feats = ms.shape
    width = feats // CHUNKS
    far_count = groups - 1
    long_count = pinc.shape[0] - 3
    tiles = live.shape[2]
    peers = [partner(g, r, groups) for r in range(1, groups)]
    order = list(reversed(range(far_count)))
    relay = groups == 4
    halves = fsend.shape[2]
    piece_rows = rows // halves
    if groups & (groups - 1):
        greeted = [to for to, _ in peers] + [source for _, source in peers]
    else:
        greeted = [to for to, _ in peers]
    not_first, not_last = d > 0, d < devs - 1
    sides = ((not_first, d - 1), (not_last, d + 1))
    far_side = lax.rem(d, 2)
    near_side = 1 - far_side
    even, odd = lax.rem(d, 2) == 0, lax.rem(d, 2) == 1

    def load(index, pairs, whole):
        starts = [pltpu.make_async_copy(src, dst, load_sem.at[index]) for src, dst in pairs]
        return starts, pltpu.make_async_copy(whole, whole, load_sem.at[index])

    far_inc, near_inc = inc.at[pl.ds(0, long_count)], inc.at[pl.ds(long_count, 3)]
    first = load(0, [(ee_h, wt.at[0])], wt.at[0])
    far_load = load(1, [(ef_h, far_inc)], far_inc)
    near_load = load(2, [(en_h, near_inc)], near_inc)
    live_load = load(3, [(el_h, live.at[0]), (dl_h, live.at[1])], live)
    region_load = load(4, [(eg_h, regions.at[0]), (pg_h, regions.at[1])], regions)
    late = [
        load(5, [(mesh_h, ms)], ms),
        load(6, [(h, wt.at[1 + i]) for i, h in enumerate((e1_h, e2_h, pe_h, p1_h, p2_h, de_h))], wt.at[pl.ds(1, 6)]),
        load(7, [(pn_h, pinc.at[pl.ds(0, 3)]), (pf_h, pinc.at[pl.ds(3, long_count)])], pinc),
        load(8, [(dn_h, dn)], dn),
        load(9, [(d1_h, dw.at[0]), (d2_h, dw.at[1])], dw),
    ]

    def start_load(loads):
        for copy in loads[0]:
            copy.start()

    cut = gs.shape[0] // GRID_CUT
    grid_rows = [pl.ds(0, cut), pl.ds(cut, gs.shape[0] - cut)]
    count = len(grid_rows)
    grid_loads = [pltpu.make_async_copy(grid_h.at[at], gs.at[at], grid_sem.at[i]) for i, at in enumerate(grid_rows)]
    start_load(first)
    for copy in grid_loads:
        copy.start()
    for loads in (region_load, far_load, live_load, near_load):
        start_load(loads)

    barrier = pltpu.get_barrier_semaphore()
    for to in greeted:
        pl.semaphore_signal(barrier, inc=1, device_id=(to, d), device_id_type=pl.DeviceIdType.MESH)
    for there, near in sides:
        @pl.when(there)
        def _():
            pl.semaphore_signal(barrier, inc=1, device_id=(g, near), device_id_type=pl.DeviceIdType.MESH)

    for side, (there, _) in enumerate(sides):
        @pl.when(jnp.logical_not(there))
        def _():
            for buf in (nrecv, mnrecv, dnrecv):
                for c in range(CHUNKS):
                    buf[side, c] = jnp.zeros((rows, width), BF16)

    if relay:
        @pl.when(odd)
        def _():
            for c in range(ODD_RS):
                frecv[c, 2] = jnp.zeros(frecv.shape[2:], BF16)

    def remote(src, dst, send, recv, to):
        return pltpu.make_async_remote_copy(
            src_ref=src, dst_ref=dst, send_sem=send, recv_sem=recv, device_id=to, device_id_type=pl.DeviceIdType.MESH
        )

    def whole(ref, send, recv):
        return remote(ref, ref, send, recv, (peers[0][0], d))

    def hand_over(phase):
        @pl.when(not_last)
        def _():
            pl.semaphore_signal(turn.at[phase], inc=1, device_id=(g, d + 1), device_id_type=pl.DeviceIdType.MESH)

    def first_axis(h):
        return h % 2

    def far_copy(c, h, kind):
        if not relay:
            return remote(fsend.at[c, kind, h], frecv.at[c, kind, h], fs_sem.at[c], fr_sem.at[c], (peers[kind][0], d))
        to = first_axis(h) if kind < 2 else 1 - first_axis(h)
        if kind == 0:
            return remote(fsend.at[c, 0, h], frelay.at[c, h], fs_sem.at[c], fl_sem.at[c, h], (peers[to][0], d))
        return remote(fsend.at[c, kind, h], frecv.at[c, kind - 1, h], fs_sem.at[c], fr_sem.at[c], (peers[to][0], d))

    def far_direct(c):
        return remote(fsend.at[c, 0], frecv.at[c, 2], fs_sem.at[CHUNKS if c else 0], fr_sem.at[c], (peers[2][0], d))

    def mfar_direct(c):
        return remote(msend.at[c], mfrecv.at[c, 2], mfs_sem.at[c], mfr_sem.at[c, 1], (peers[2][0], d))

    def near_copy(c, s):
        return remote(nsend.at[s, c], nrecv.at[1 - s, c], ns_sem.at[s], nr_sem.at[1 - s], (g, sides[s][1]))

    def mfar_copy(c, h, i):
        at = pl.ds(h * piece_rows, piece_rows)
        source, to, recv = msend.at[c, at], i, mfr_sem.at[c, 0]
        if relay:
            if i == 2:
                source, to, recv = mfrecv.at[c, first_axis(h), at], 1 - first_axis(h), mfr_sem.at[c, 1]
            elif i == first_axis(h) and c < ODD_AG:
                recv = mfl_sem.at[c, h]
        return remote(source, mfrecv.at[c, i, at], mfs_sem.at[c], recv, (peers[to][0], d))

    def mnear_copy(c, s):
        return remote(msend.at[c], mnrecv.at[1 - s, c], mns_sem.at[s], mnr_sem.at[1 - s], (g, sides[s][1]))

    def dec_copy(c, s):
        return remote(dsend.at[c], dnrecv.at[1 - s, c], ds_sem.at[s], dr_sem.at[1 - s, c], (g, sides[s][1]))

    def start_side(copy, c):
        for s, (there, _) in enumerate(sides):
            @pl.when(there)
            def _():
                copy(c, s).start()

    def wait_side(buf, sem, s):
        @pl.when(sides[s][0])
        def _():
            whole(buf.at[s], sem.at[s], sem.at[s]).wait_recv()

    greetings = len(greeted) + jnp.where(not_first, 1, 0) + jnp.where(not_last, 1, 0)
    with scope("ldwait"):
        first[1].wait()
    for c in range(CHUNKS):
        cols = pl.ds(c * width, width)
        for i in range(count):
            if c == 0:
                with scope("gridwait"):
                    grid_loads[i].wait()
                    if i == count - 1:
                        region_load[1].wait()
                        far_load[1].wait()
                        pl.semaphore_wait(barrier, greetings)
            at = grid_rows[i]
            em[c, at, :] = silu(mm(gs[at, :], wt[0, :, cols])).astype(BF16)
        far_all = mm(inc[pl.ds(0, long_count)].reshape(long_count * rows, gs.shape[0]), em[c])
        far = [far_all[i * rows:(i + 1) * rows] for i in range(long_count)]

        def toward(i):
            total = None
            for index in range(long_count):
                flag = jnp.where(regions[0, 0, index] == peers[i][0], 1.0, 0.0).astype(F32)
                term = far[index] * flag
                total = term if total is None else total + term
            return total

        if relay:
            totals = [toward(i) for i in range(far_count)]
            for kind in range(2):
                for h in range(halves):
                    at = slice(h * piece_rows, (h + 1) * piece_rows)
                    axis = first_axis(h)
                    fsend[c, kind, h] = totals[2 if kind == 0 else axis][at].astype(BF16)
                    if kind == 0:
                        fheld[c, h] = totals[1 - axis][at]
                        if True:
                            fsend[c, 2, h] = totals[1 - axis][at].astype(BF16)

            @pl.when(even)
            def _():
                far_direct(c).start()
                for kind in (1, 2):
                    for h in range(halves):
                        far_copy(c, h, kind).start()

        else:
            for i in order:
                fsend[c, i, 0] = toward(i).astype(BF16)
                far_copy(c, 0, i).start()

    for loads in late:
        start_load(loads)
    with scope("enwait"):
        live_load[1].wait()
        near_load[1].wait()
    for k in range(3):
        for t in range(tiles):
            flag = live[0, k, t].astype(F32).astype(BF16)
            at = pl.ds(t * rows, rows)
            inc[long_count + k, :, at] = inc[long_count + k, :, at] * flag
    for c in range(CHUNKS):
        cols = pl.ds(c * width, width)
        near_all = mm(inc[pl.ds(long_count, 3)].reshape(3 * rows, gs.shape[0]), em[c])
        for s, k in ((0, 0), (1, 2)):
            nsend[s, c] = near_all[k * rows:(k + 1) * rows].astype(BF16)
        start_side(near_copy, c)
        own_near[:, cols] = near_all[rows:2 * rows].astype(BF16)

    if relay:
        @pl.when(even)
        def _():
            with scope("rsdrain"):
                whole(fsend.at[0], fs_sem.at[0], fs_sem.at[0]).wait_send()
                whole(fsend.at[1, 0], fs_sem.at[CHUNKS], fs_sem.at[CHUNKS]).wait_send()
            hand_over(0)

        @pl.when(odd)
        def _():
            with scope("rsturn"):
                pl.semaphore_wait(turn.at[0], 1)
            for c in range(ODD_RS):
                for h in range(halves):
                    far_copy(c, h, 0).start()
            for c in range(ODD_RS, CHUNKS):
                far_direct(c).start()
            for c in range(CHUNKS):
                for kind in (1, 2) if c >= ODD_RS else (1,):
                    for h in range(halves):
                        far_copy(c, h, kind).start()

        def pass_on(c):
            for h in range(halves):
                with scope("relaywait"):
                    far_copy(c, h, 0).wait_recv()
                fsend[c, 2, h] = (fheld[c, h] + frelay[c, h].astype(F32)).astype(BF16)
                far_copy(c, h, 2).start()

        for c in range(ODD_RS):
            pl.when(odd)(functools.partial(pass_on, c))

    for loads in late:
        loads[1].wait()
    for i in range(far_count):
        total = None
        for index in range(long_count):
            flag = jnp.where(regions[1, 0, index] == peers[i][1], 1.0, 0.0).astype(F32)
            term = pinc[3 + index].astype(F32) * flag
            total = term if total is None else total + term
        proc_inc[i] = total.astype(BF16)
    for k in range(3):
        for t in range(tiles):
            at = pl.ds(t * rows, rows)
            dn[k, at, :] = dn[k, at, :] * live[1, k, t].astype(F32).astype(BF16)

    def node_update(residual, summed, first, second):
        cent, half = centred(summed)
        hidden = gate(half * mm(cent, wt[first])).astype(BF16)
        return (residual.astype(F32) + mm(hidden, wt[second])).astype(BF16)

    with scope("nearwait"):
        for s in range(2):
            wait_side(nrecv, nr_sem, s)
    parts = []
    for c in range(CHUNKS):
        total = own_near[:, pl.ds(c * width, width)].astype(F32)
        for s in range(2):
            total = total + nrecv[s, c].astype(F32)
        slots = far_count
        with scope("farwait"):
            if relay and c < ODD_RS:
                @pl.when(even)
                def _():
                    whole(frecv.at[c], fr_sem.at[c], fr_sem.at[c]).wait_recv()

                @pl.when(odd)
                def _():
                    whole(frecv.at[c, pl.ds(0, 2)], fr_sem.at[c], fr_sem.at[c]).wait_recv()
            else:
                whole(frecv.at[c, pl.ds(0, slots)], fr_sem.at[c], fr_sem.at[c]).wait_recv()
        pieces = []
        for h in range(halves):
            piece = total[h * piece_rows:(h + 1) * piece_rows]
            for i in range(slots):
                piece = piece + frecv[c, i, h].astype(F32)
            pieces.append(piece)
        parts.append(jnp.concatenate(pieces, axis=0))
    with scope("upd1"):
        mesh_mid = node_update(ms[...], jnp.concatenate(parts, axis=1), 1, 2)

    for c in range(CHUNKS):
        msend[c] = silu(mm(mesh_mid, wt[3, :, pl.ds(c * width, width)])).astype(BF16)
        if not relay:
            for i in order:
                mfar_copy(c, 0, i).start()
        else:
            @pl.when(even)
            def _():
                mfar_direct(c).start()
                for h in range(halves):
                    mfar_copy(c, h, first_axis(h)).start()
                    mfar_copy(c, h, 1 - first_axis(h)).start()
        start_side(mnear_copy, c)

    def send_second():
        for c in range(CHUNKS):
            for h in range(halves):
                mfar_copy(c, h, 1 - first_axis(h)).start()

    if relay:
        @pl.when(odd)
        def _():
            with scope("oddwait"):
                pl.semaphore_wait(turn.at[1], 1)
            for h in range(halves):
                mfar_copy(0, h, first_axis(h)).start()
            for c in range(ODD_AG, CHUNKS):
                mfar_direct(c).start()
            for h in range(halves):
                mfar_copy(1, h, first_axis(h)).start()
            for h in range(halves):
                mfar_copy(0, h, 1 - first_axis(h)).start()
    parts = [mm(pinc[1], msend[c]) for c in range(CHUNKS)]
    if relay:
        @pl.when(even)
        def _():
            with scope("agdrain"):
                whole(mfrecv.at[0], mfs_sem.at[0], mfs_sem.at[0]).wait_send()
            hand_over(1)
    if relay:
        for c in range(ODD_AG):
            for h in range(halves):
                with scope("mrelaywait"):
                    mfar_copy(c, h, first_axis(h)).wait_recv()

                @pl.when(odd)
                def _():
                    mfar_copy(c, h, 2).start()

        @pl.when(odd)
        def _():
            for h in range(halves):
                mfar_copy(1, h, 1 - first_axis(h)).start()
    for s in range(2):
        with scope("mnearwait"):
            wait_side(mnrecv, mnr_sem, s)
        for c in range(CHUNKS):
            parts[c] = parts[c] + mm(pinc[2 * s], mnrecv[s, c])
    for c in range(CHUNKS):
        with scope("mfarwait"):
            if relay:
                own = mfrecv.at[c, 0] if c < ODD_AG else mfrecv.at[c, pl.ds(0, 2)]
                whole(own, mfr_sem.at[c, 0], mfr_sem.at[c, 0]).wait_recv()
            else:
                whole(mfrecv.at[c], mfr_sem.at[c, 0], mfr_sem.at[c, 0]).wait_recv()
        for i in range(2 if relay else far_count):
            parts[c] = parts[c] + mm(proc_inc[i], mfrecv[c, i])
    if relay:
        for c in range(CHUNKS):
            with scope("mdiagwait"):
                whole(mfrecv.at[c, 2], mfr_sem.at[c, 1], mfr_sem.at[c, 1]).wait_recv()
            parts[c] = parts[c] + mm(proc_inc[2], mfrecv[c, 2])
    with scope("upd2"):
        mesh_next = node_update(mesh_mid, jnp.concatenate(parts, axis=1), 4, 5)
    mesh_out[...] = mesh_next

    for c in range(CHUNKS):
        dsend[c] = silu(mm(mesh_next, wt[6, :, pl.ds(c * width, width)])).astype(BF16)
        start_side(dec_copy, c)

    block = 2 * rows

    def decode(add, c, k, source):
        for i in range(gs.shape[0] // block):
            at = pl.ds(i * block, block)
            part = mm(dn[k, at, :], source)
            acc[at, pl.ds(c * width, width)] = acc[at, pl.ds(c * width, width)] + part if add else part

    with scope("ownpart"):
        for c in range(CHUNKS):
            decode(False, c, 1, dsend[c])
    for s in (near_side, far_side):
        there = jnp.where(s == 0, not_first, not_last)
        for c in range(CHUNKS):
            with scope("decwait"):
                @pl.when(there)
                def _():
                    whole(dnrecv.at[s, c], dr_sem.at[s, c], dr_sem.at[s, c]).wait_recv()
            if s is near_side or c < CHUNKS - 1:
                decode(True, c, 2 * s, dnrecv[s, c])
    last[...] = dnrecv[far_side, CHUNKS - 1]

    with scope("drain"):
        def far_sent(c):
            sent = fsend.at[c, pl.ds(1, 2)] if relay and c else fsend.at[c]
            whole(sent, fs_sem.at[c], fs_sem.at[c]).wait_send()
            whole(mfrecv.at[c], mfs_sem.at[c], mfs_sem.at[c]).wait_send()
            if relay and c == 0:
                whole(fsend.at[1, 0], fs_sem.at[CHUNKS], fs_sem.at[CHUNKS]).wait_send()

        for c in range(CHUNKS):
            if relay and c == 0:
                pl.when(odd)(functools.partial(far_sent, c))
            else:
                far_sent(c)
        for s, (there, _) in enumerate(sides):
            @pl.when(there)
            def _():
                whole(nsend.at[s], ns_sem.at[s], ns_sem.at[s]).wait_send()
                whole(msend, mns_sem.at[s], mns_sem.at[s]).wait_send()
                whole(dsend, ds_sem.at[s], ds_sem.at[s]).wait_send()


def finish(mesh_v, gs, dw, acc, dn, last, grid_o, mesh_o, grid_out, out_sem):
    step = gs.shape[0] // (out_sem.shape[0] - 1)
    width = gs.shape[1] // CHUNKS
    side = lax.rem(lax.axis_index("dev"), 2)
    mesh_copy = pltpu.make_async_copy(mesh_v, mesh_o, out_sem.at[0])
    mesh_copy.start()
    outs = []
    for i in range(gs.shape[0] // step):
        at = pl.ds(i * step, step)
        held = [acc[at, pl.ds(c * width, width)] for c in range(CHUNKS)]
        held[-1] = held[-1] + mm(dn[2 * side, at, :], last[...])
        cent, half = centred(jnp.concatenate(held, axis=1))
        parts = [gate(half * mm(cent, dw[0, :, pl.ds(c * width, width)])).astype(BF16) for c in range(CHUNKS)]
        hidden = jnp.concatenate(parts, axis=1)
        for c in range(CHUNKS):
            cols = pl.ds(c * width, width)
            grid_out[at, cols] = (gs[at, cols].astype(F32) + mm(hidden, dw[1, :, cols])).astype(BF16)
        copy = pltpu.make_async_copy(grid_out.at[at], grid_o.at[at], out_sem.at[1 + i])
        copy.start()
        outs.append(copy)
    with scope("outwait"):
        mesh_copy.wait()
        for copy in outs:
            copy.wait()


def body(groups, devs, *args):
    grid_state, mesh_state = args[0], args[1]
    args = list(args)
    args[14], args[17] = args[14].T, args[17].T
    encode_live, encode_far, encode_groups, decode_near = args[12], args[13], args[14], args[18]
    grid_rows, feats = grid_state.shape
    rows = mesh_state.shape[0]
    width = feats // CHUNKS
    far_count = groups - 1
    long_count = encode_far.shape[0]

    def vmem(*shape, dtype=BF16):
        return pltpu.VMEM(shape, dtype)

    dma = pltpu.SemaphoreType.DMA
    relay = groups == 4
    halves = 2 if relay else 1
    piece = (rows // halves, width)
    block = (rows, width)
    scratch = [
        vmem(rows, feats), vmem(7, feats, feats), vmem(3 + long_count, rows, grid_rows),
        pltpu.SMEM((2, *encode_live.shape), jnp.int32), pltpu.SMEM((2, *encode_groups.shape), jnp.int32),
        vmem(3 + long_count, rows, rows),
        vmem(CHUNKS, grid_rows, width),
        vmem(CHUNKS, halves, *piece, dtype=F32), vmem(CHUNKS, far_count, halves, *piece),
        vmem(CHUNKS, halves, *piece), vmem(CHUNKS, far_count, halves, *piece),
        vmem(2, CHUNKS, *block), vmem(2, CHUNKS, *block),
        vmem(CHUNKS, *block), vmem(CHUNKS, far_count, *block), vmem(2, CHUNKS, *block),
        vmem(CHUNKS, *block), vmem(2, CHUNKS, *block),
        vmem(rows, feats), vmem(far_count, rows, rows),
        dma((10,)), dma((2,)), dma((CHUNKS + 1,)), dma((ODD_RS, halves)), dma((CHUNKS,)), dma((2,)), dma((2,)),
        dma((CHUNKS,)), dma((ODD_AG, halves)), dma((CHUNKS, 2)), dma((2,)), dma((2,)), dma((2,)), dma((2, CHUNKS)), pltpu.SemaphoreType.REGULAR((2,)),
    ]
    hbm = pl.BlockSpec(memory_space=pltpu.HBM)
    on_chip = pl.BlockSpec(memory_space=pltpu.VMEM)
    held = pl.pallas_call(
        functools.partial(exchange, groups, devs),
        out_shape=(
            vmem(*mesh_state.shape), vmem(*grid_state.shape), vmem(2, feats, feats), vmem(*grid_state.shape, dtype=F32),
            vmem(*decode_near.shape), vmem(*block),
        ),
        in_specs=[hbm] * len(args),
        out_specs=(on_chip,) * 6,
        scratch_shapes=scratch,
        compiler_params=pltpu.CompilerParams(collective_id=0, has_side_effects=True, vmem_limit_bytes=32 << 20),
        name="exchange",
    )(*(pltpu.with_memory_space_constraint(arg, pltpu.HBM) for arg in args))
    return pl.pallas_call(
        finish,
        out_shape=(
            jax.ShapeDtypeStruct(grid_state.shape, BF16),
            jax.ShapeDtypeStruct(mesh_state.shape, BF16),
        ),
        in_specs=[on_chip] * 6,
        out_specs=(hbm, hbm),
        scratch_shapes=[vmem(*grid_state.shape), dma((1 + GRID_OUTS,))],
        compiler_params=pltpu.CompilerParams(vmem_limit_bytes=16 << 20),
        name="finish",
    )(*held)


def solution(mesh):
    both = ("group", "dev")
    row, whole, second = P(both, None), P(), P(None, both, None)
    flags = P(None, both)
    return jax.shard_map(
        functools.partial(body, mesh.shape["group"], mesh.shape["dev"]),
        mesh=mesh,
        in_specs=(
            row, row, whole, whole, whole, whole, whole, whole, whole, whole, whole,
            second, flags, second, flags, second, second, flags, second, flags,
        ),
        out_specs=(row, row),
        check_vma=False,
    )
```

```python
import contextlib
import functools

import jax
import jax.numpy as jnp
from jax import lax
from jax.experimental import pallas as pl
from jax.experimental.pallas import tpu as pltpu
from jax.sharding import PartitionSpec as P

BF16 = jnp.bfloat16
F32 = jnp.float32
CHUNKS = 2
GRID_CUT = 4
GRID_OUTS = 2
ODD_RS = 1
ODD_AG = 1


def gate(half):
    return half + half * jnp.tanh(half)


def silu(x):
    return gate(0.5 * x)


def mm(a, b):
    return jnp.dot(a, b, preferred_element_type=F32)


def centred(v):
    cent = v - jnp.mean(v, axis=-1, keepdims=True)
    var = jnp.mean(cent * cent, axis=-1, keepdims=True)
    return cent.astype(BF16), 0.5 * lax.rsqrt(var + 1e-05)


def partner(me, r, count):
    if count & (count - 1):
        return lax.rem(me + r, count), lax.rem(me + count - r, count)
    out, bit = me, 1
    while bit < count:
        if r & bit:
            out = out + bit * (1 - 2 * lax.rem(me // bit, 2))
        bit *= 2
    return out, out


def scope(name):
    return contextlib.nullcontext()


def exchange(
    groups,
    devs,
    grid_h, mesh_h, ee_h, e1_h, e2_h, pe_h, p1_h, p2_h, de_h, d1_h, d2_h,
    en_h, el_h, ef_h, eg_h, pn_h, pf_h, pg_h, dn_h, dl_h,
    mesh_out, gs, dw, acc,
    ms, wt, inc, live, regions, pinc, dn,
    em, fheld, fsend, frelay, frecv, nsend, nrecv, msend, mfrecv, mnrecv, dsend, dnrecv,
    own_near, proc_inc,
    load_sem, grid_sem, fs_sem, fl_sem, fr_sem, ns_sem, nr_sem, mfs_sem, mfl_sem, mfr_sem, mns_sem, mnr_sem, ds_sem, dr_sem, turn,
):
    g = lax.axis_index("group")
    d = lax.axis_index("dev")
    rows, feats = ms.shape
    width = feats // CHUNKS
    far_count = groups - 1
    long_count = pinc.shape[0] - 3
    tiles = live.shape[2]
    peers = [partner(g, r, groups) for r in range(1, groups)]
    order = list(reversed(range(far_count)))
    relay = groups == 4
    halves = fsend.shape[2]
    piece_rows = rows // halves
    if groups & (groups - 1):
        greeted = [to for to, _ in peers] + [source for _, source in peers]
    else:
        greeted = [to for to, _ in peers]
    not_first, not_last = d > 0, d < devs - 1
    sides = ((not_first, d - 1), (not_last, d + 1))
    far_side = lax.rem(d, 2)
    near_side = 1 - far_side
    even, odd = lax.rem(d, 2) == 0, lax.rem(d, 2) == 1

    def load(index, pairs, whole):
        starts = [pltpu.make_async_copy(src, dst, load_sem.at[index]) for src, dst in pairs]
        return starts, pltpu.make_async_copy(whole, whole, load_sem.at[index])

    far_inc, near_inc = inc.at[pl.ds(0, long_count)], inc.at[pl.ds(long_count, 3)]
    first = load(0, [(ee_h, wt.at[0])], wt.at[0])
    far_load = load(1, [(ef_h, far_inc)], far_inc)
    near_load = load(2, [(en_h, near_inc)], near_inc)
    live_load = load(3, [(el_h, live.at[0]), (dl_h, live.at[1])], live)
    region_load = load(4, [(eg_h, regions.at[0]), (pg_h, regions.at[1])], regions)
    late = [
        load(5, [(mesh_h, ms)], ms),
        load(6, [(h, wt.at[1 + i]) for i, h in enumerate((e1_h, e2_h, pe_h, p1_h, p2_h, de_h))], wt.at[pl.ds(1, 6)]),
        load(7, [(pn_h, pinc.at[pl.ds(0, 3)]), (pf_h, pinc.at[pl.ds(3, long_count)])], pinc),
        load(8, [(dn_h, dn)], dn),
        load(9, [(d1_h, dw.at[0]), (d2_h, dw.at[1])], dw),
    ]

    def start_load(loads):
        for copy in loads[0]:
            copy.start()

    cut = gs.shape[0] // GRID_CUT
    grid_rows = [pl.ds(0, cut), pl.ds(cut, gs.shape[0] - cut)]
    count = len(grid_rows)
    grid_loads = [pltpu.make_async_copy(grid_h.at[at], gs.at[at], grid_sem.at[i]) for i, at in enumerate(grid_rows)]
    start_load(first)
    for copy in grid_loads:
        copy.start()
    for loads in (region_load, far_load, live_load, near_load):
        start_load(loads)

    barrier = pltpu.get_barrier_semaphore()
    for to in greeted:
        pl.semaphore_signal(barrier, inc=1, device_id=(to, d), device_id_type=pl.DeviceIdType.MESH)
    for there, near in sides:
        @pl.when(there)
        def _():
            pl.semaphore_signal(barrier, inc=1, device_id=(g, near), device_id_type=pl.DeviceIdType.MESH)

    for side, (there, _) in enumerate(sides):
        @pl.when(jnp.logical_not(there))
        def _():
            for buf in (nrecv, mnrecv, dnrecv):
                for c in range(CHUNKS):
                    buf[side, c] = jnp.zeros((rows, width), BF16)

    if relay:
        @pl.when(odd)
        def _():
            for c in range(ODD_RS):
                frecv[c, 2] = jnp.zeros(frecv.shape[2:], BF16)

    def remote(src, dst, send, recv, to):
        return pltpu.make_async_remote_copy(
            src_ref=src, dst_ref=dst, send_sem=send, recv_sem=recv, device_id=to, device_id_type=pl.DeviceIdType.MESH
        )

    def whole(ref, send, recv):
        return remote(ref, ref, send, recv, (peers[0][0], d))

    def hand_over(phase):
        @pl.when(not_last)
        def _():
            pl.semaphore_signal(turn.at[phase], inc=1, device_id=(g, d + 1), device_id_type=pl.DeviceIdType.MESH)

    def first_axis(h):
        return h % 2

    def far_copy(c, h, kind):
        if not relay:
            return remote(fsend.at[c, kind, h], frecv.at[c, kind, h], fs_sem.at[c], fr_sem.at[c], (peers[kind][0], d))
        to = first_axis(h) if kind < 2 else 1 - first_axis(h)
        if kind == 0:
            return remote(fsend.at[c, 0, h], frelay.at[c, h], fs_sem.at[c], fl_sem.at[c, h], (peers[to][0], d))
        return remote(fsend.at[c, kind, h], frecv.at[c, kind - 1, h], fs_sem.at[c], fr_sem.at[c], (peers[to][0], d))

    def far_direct(c):
        return remote(fsend.at[c, 0], frecv.at[c, 2], fs_sem.at[CHUNKS if c else 0], fr_sem.at[c], (peers[2][0], d))

    def mfar_direct(c):
        return remote(msend.at[c], mfrecv.at[c, 2], mfs_sem.at[CHUNKS if c else 0], mfr_sem.at[c, 1], (peers[2][0], d))

    def near_copy(c, s):
        return remote(nsend.at[s, c], nrecv.at[1 - s, c], ns_sem.at[s], nr_sem.at[1 - s], (g, sides[s][1]))

    def mfar_copy(c, h, i):
        at = pl.ds(h * piece_rows, piece_rows)
        source, to, recv = msend.at[c, at], i, mfr_sem.at[c, 0]
        if relay:
            if i == 2:
                source, to, recv = mfrecv.at[c, first_axis(h), at], 1 - first_axis(h), mfr_sem.at[c, 1]
            elif i == first_axis(h) and c < ODD_AG:
                recv = mfl_sem.at[c, h]
        return remote(source, mfrecv.at[c, i, at], mfs_sem.at[c], recv, (peers[to][0], d))

    def mnear_copy(c, s):
        return remote(msend.at[c], mnrecv.at[1 - s, c], mns_sem.at[s], mnr_sem.at[1 - s], (g, sides[s][1]))

    def dec_copy(c, s):
        return remote(dsend.at[c], dnrecv.at[1 - s, c], ds_sem.at[s], dr_sem.at[1 - s, c], (g, sides[s][1]))

    def start_side(copy, c):
        for s, (there, _) in enumerate(sides):
            @pl.when(there)
            def _():
                copy(c, s).start()

    def wait_side(buf, sem, s):
        @pl.when(sides[s][0])
        def _():
            whole(buf.at[s], sem.at[s], sem.at[s]).wait_recv()

    greetings = len(greeted) + jnp.where(not_first, 1, 0) + jnp.where(not_last, 1, 0)
    with scope("ldwait"):
        first[1].wait()
    for c in range(CHUNKS):
        cols = pl.ds(c * width, width)
        for i in range(count):
            if c == 0:
                with scope("gridwait"):
                    grid_loads[i].wait()
                    if i == count - 1:
                        region_load[1].wait()
                        far_load[1].wait()
                        pl.semaphore_wait(barrier, greetings)
            at = grid_rows[i]
            em[c, at, :] = silu(mm(gs[at, :], wt[0, :, cols])).astype(BF16)
        far_all = mm(inc[pl.ds(0, long_count)].reshape(long_count * rows, gs.shape[0]), em[c])
        far = [far_all[i * rows:(i + 1) * rows] for i in range(long_count)]

        def toward(i):
            total = None
            for index in range(long_count):
                flag = jnp.where(regions[0, 0, index] == peers[i][0], 1.0, 0.0).astype(F32)
                term = far[index] * flag
                total = term if total is None else total + term
            return total

        if relay:
            totals = [toward(i) for i in range(far_count)]
            for kind in range(2):
                for h in range(halves):
                    at = slice(h * piece_rows, (h + 1) * piece_rows)
                    axis = first_axis(h)
                    fsend[c, kind, h] = totals[2 if kind == 0 else axis][at].astype(BF16)
                    if kind == 0:
                        fheld[c, h] = totals[1 - axis][at]
                        if True:
                            fsend[c, 2, h] = totals[1 - axis][at].astype(BF16)

            @pl.when(even)
            def _():
                far_direct(c).start()
                for kind in (1, 2):
                    for h in range(halves):
                        far_copy(c, h, kind).start()

        else:
            for i in order:
                fsend[c, i, 0] = toward(i).astype(BF16)
                far_copy(c, 0, i).start()

    for loads in late:
        start_load(loads)
    with scope("enwait"):
        live_load[1].wait()
        near_load[1].wait()
    for k in range(3):
        for t in range(tiles):
            flag = live[0, k, t].astype(F32).astype(BF16)
            at = pl.ds(t * rows, rows)
            inc[long_count + k, :, at] = inc[long_count + k, :, at] * flag
    for c in range(CHUNKS):
        cols = pl.ds(c * width, width)
        near_all = mm(inc[pl.ds(long_count, 3)].reshape(3 * rows, gs.shape[0]), em[c])
        for s, k in ((0, 0), (1, 2)):
            nsend[s, c] = near_all[k * rows:(k + 1) * rows].astype(BF16)
        start_side(near_copy, c)
        own_near[:, cols] = near_all[rows:2 * rows].astype(BF16)

    if relay:
        @pl.when(even)
        def _():
            with scope("rsdrain"):
                whole(fsend.at[0], fs_sem.at[0], fs_sem.at[0]).wait_send()
                whole(fsend.at[1, 0], fs_sem.at[CHUNKS], fs_sem.at[CHUNKS]).wait_send()
            hand_over(0)

        @pl.when(odd)
        def _():
            with scope("rsturn"):
                pl.semaphore_wait(turn.at[0], 1)
            for c in range(ODD_RS):
                for h in range(halves):
                    far_copy(c, h, 0).start()
            for c in range(ODD_RS, CHUNKS):
                far_direct(c).start()
            for c in range(CHUNKS):
                for kind in (1, 2) if c >= ODD_RS else (1,):
                    for h in range(halves):
                        far_copy(c, h, kind).start()

        def pass_on(c):
            for h in range(halves):
                with scope("relaywait"):
                    far_copy(c, h, 0).wait_recv()
                fsend[c, 2, h] = (fheld[c, h] + frelay[c, h].astype(F32)).astype(BF16)
                far_copy(c, h, 2).start()

        for c in range(ODD_RS):
            pl.when(odd)(functools.partial(pass_on, c))

    for loads in late:
        loads[1].wait()
    for i in range(far_count):
        total = None
        for index in range(long_count):
            flag = jnp.where(regions[1, 0, index] == peers[i][1], 1.0, 0.0).astype(F32)
            term = pinc[3 + index].astype(F32) * flag
            total = term if total is None else total + term
        proc_inc[i] = total.astype(BF16)
    for k in range(3):
        for t in range(tiles):
            at = pl.ds(t * rows, rows)
            dn[k, at, :] = dn[k, at, :] * live[1, k, t].astype(F32).astype(BF16)

    def node_update(residual, summed, first, second):
        cent, half = centred(summed)
        hidden = gate(half * mm(cent, wt[first])).astype(BF16)
        return (residual.astype(F32) + mm(hidden, wt[second])).astype(BF16)

    with scope("nearwait"):
        for s in range(2):
            wait_side(nrecv, nr_sem, s)
    parts = []
    for c in range(CHUNKS):
        total = own_near[:, pl.ds(c * width, width)].astype(F32)
        for s in range(2):
            total = total + nrecv[s, c].astype(F32)
        slots = far_count
        with scope("farwait"):
            if relay and c < ODD_RS:
                @pl.when(even)
                def _():
                    whole(frecv.at[c], fr_sem.at[c], fr_sem.at[c]).wait_recv()

                @pl.when(odd)
                def _():
                    whole(frecv.at[c, pl.ds(0, 2)], fr_sem.at[c], fr_sem.at[c]).wait_recv()
            else:
                whole(frecv.at[c, pl.ds(0, slots)], fr_sem.at[c], fr_sem.at[c]).wait_recv()
        pieces = []
        for h in range(halves):
            piece = total[h * piece_rows:(h + 1) * piece_rows]
            for i in range(slots):
                piece = piece + frecv[c, i, h].astype(F32)
            pieces.append(piece)
        parts.append(jnp.concatenate(pieces, axis=0))
    with scope("upd1"):
        mesh_mid = node_update(ms[...], jnp.concatenate(parts, axis=1), 1, 2)

    for c in range(CHUNKS):
        msend[c] = silu(mm(mesh_mid, wt[3, :, pl.ds(c * width, width)])).astype(BF16)
        if not relay:
            for i in order:
                mfar_copy(c, 0, i).start()
        else:
            @pl.when(even)
            def _():
                mfar_direct(c).start()
                for h in range(halves):
                    mfar_copy(c, h, first_axis(h)).start()
                    mfar_copy(c, h, 1 - first_axis(h)).start()
        start_side(mnear_copy, c)

    def send_second():
        for c in range(CHUNKS):
            for h in range(halves):
                mfar_copy(c, h, 1 - first_axis(h)).start()

    if relay:
        @pl.when(odd)
        def _():
            with scope("oddwait"):
                pl.semaphore_wait(turn.at[1], 1)
            for h in range(halves):
                mfar_copy(0, h, first_axis(h)).start()
            for c in range(ODD_AG, CHUNKS):
                mfar_direct(c).start()
            for h in range(halves):
                mfar_copy(1, h, first_axis(h)).start()
            for h in range(halves):
                mfar_copy(0, h, 1 - first_axis(h)).start()
    parts = [mm(pinc[1], msend[c]) for c in range(CHUNKS)]
    if relay:
        @pl.when(even)
        def _():
            with scope("agdrain"):
                whole(mfrecv.at[0], mfs_sem.at[0], mfs_sem.at[0]).wait_send()
                whole(msend.at[1], mfs_sem.at[CHUNKS], mfs_sem.at[CHUNKS]).wait_send()
            hand_over(1)
    if relay:
        for c in range(ODD_AG):
            for h in range(halves):
                with scope("mrelaywait"):
                    mfar_copy(c, h, first_axis(h)).wait_recv()

                @pl.when(odd)
                def _():
                    mfar_copy(c, h, 2).start()

        @pl.when(odd)
        def _():
            for h in range(halves):
                mfar_copy(1, h, 1 - first_axis(h)).start()
    for s in range(2):
        with scope("mnearwait"):
            wait_side(mnrecv, mnr_sem, s)
        for c in range(CHUNKS):
            parts[c] = parts[c] + mm(pinc[2 * s], mnrecv[s, c])
    for c in range(CHUNKS):
        with scope("mfarwait"):
            if relay:
                own = mfrecv.at[c, 0] if c < ODD_AG else mfrecv.at[c, pl.ds(0, 2)]
                whole(own, mfr_sem.at[c, 0], mfr_sem.at[c, 0]).wait_recv()
            else:
                whole(mfrecv.at[c], mfr_sem.at[c, 0], mfr_sem.at[c, 0]).wait_recv()
        for i in range(2 if relay else far_count):
            parts[c] = parts[c] + mm(proc_inc[i], mfrecv[c, i])
    if relay:
        for c in range(CHUNKS):
            with scope("mdiagwait"):
                whole(mfrecv.at[c, 2], mfr_sem.at[c, 1], mfr_sem.at[c, 1]).wait_recv()
            parts[c] = parts[c] + mm(proc_inc[2], mfrecv[c, 2])
    with scope("upd2"):
        mesh_next = node_update(mesh_mid, jnp.concatenate(parts, axis=1), 4, 5)
    mesh_out[...] = mesh_next

    for c in range(CHUNKS):
        dsend[c] = silu(mm(mesh_next, wt[6, :, pl.ds(c * width, width)])).astype(BF16)
        start_side(dec_copy, c)

    block = 2 * rows

    def decode(add, c, k, source):
        for i in range(gs.shape[0] // block):
            at = pl.ds(i * block, block)
            part = mm(dn[k, at, :], source)
            acc[at, pl.ds(c * width, width)] = acc[at, pl.ds(c * width, width)] + part if add else part

    with scope("ownpart"):
        for c in range(CHUNKS):
            decode(False, c, 1, dsend[c])
    for s in (near_side, far_side):
        there = jnp.where(s == 0, not_first, not_last)
        for c in range(CHUNKS):
            with scope("decwait"):
                @pl.when(there)
                def _():
                    whole(dnrecv.at[s, c], dr_sem.at[s, c], dr_sem.at[s, c]).wait_recv()
            decode(True, c, 2 * s, dnrecv[s, c])

    with scope("drain"):
        def far_sent(c):
            sent = fsend.at[c, pl.ds(1, 2)] if relay and c else fsend.at[c]
            whole(sent, fs_sem.at[c], fs_sem.at[c]).wait_send()
            sent = mfrecv.at[c, pl.ds(0, 2)] if relay and c else mfrecv.at[c]
            whole(sent, mfs_sem.at[c], mfs_sem.at[c]).wait_send()
            if relay and c == 0:
                whole(msend.at[1], mfs_sem.at[CHUNKS], mfs_sem.at[CHUNKS]).wait_send()
                whole(fsend.at[1, 0], fs_sem.at[CHUNKS], fs_sem.at[CHUNKS]).wait_send()

        for c in range(CHUNKS):
            if relay and c == 0:
                pl.when(odd)(functools.partial(far_sent, c))
            else:
                far_sent(c)
        for s, (there, _) in enumerate(sides):
            @pl.when(there)
            def _():
                whole(nsend.at[s], ns_sem.at[s], ns_sem.at[s]).wait_send()
                whole(msend, mns_sem.at[s], mns_sem.at[s]).wait_send()
                whole(dsend, ds_sem.at[s], ds_sem.at[s]).wait_send()


def finish(mesh_v, gs, dw, acc, grid_o, mesh_o, grid_out, out_sem):
    step = gs.shape[0] // (out_sem.shape[0] - 1)
    width = gs.shape[1] // CHUNKS
    mesh_copy = pltpu.make_async_copy(mesh_v, mesh_o, out_sem.at[0])
    mesh_copy.start()
    outs = []
    for i in range(gs.shape[0] // step):
        at = pl.ds(i * step, step)
        held = [acc[at, pl.ds(c * width, width)] for c in range(CHUNKS)]
        cent, half = centred(jnp.concatenate(held, axis=1))
        parts = [gate(half * mm(cent, dw[0, :, pl.ds(c * width, width)])).astype(BF16) for c in range(CHUNKS)]
        hidden = jnp.concatenate(parts, axis=1)
        for c in range(CHUNKS):
            cols = pl.ds(c * width, width)
            grid_out[at, cols] = (gs[at, cols].astype(F32) + mm(hidden, dw[1, :, cols])).astype(BF16)
        copy = pltpu.make_async_copy(grid_out.at[at], grid_o.at[at], out_sem.at[1 + i])
        copy.start()
        outs.append(copy)
    with scope("outwait"):
        mesh_copy.wait()
        for copy in outs:
            copy.wait()


def body(groups, devs, *args):
    grid_state, mesh_state = args[0], args[1]
    args = list(args)
    args[14], args[17] = args[14].T, args[17].T
    encode_live, encode_far, encode_groups, decode_near = args[12], args[13], args[14], args[18]
    grid_rows, feats = grid_state.shape
    rows = mesh_state.shape[0]
    width = feats // CHUNKS
    far_count = groups - 1
    long_count = encode_far.shape[0]

    def vmem(*shape, dtype=BF16):
        return pltpu.VMEM(shape, dtype)

    dma = pltpu.SemaphoreType.DMA
    relay = groups == 4
    halves = 2 if relay else 1
    piece = (rows // halves, width)
    block = (rows, width)
    scratch = [
        vmem(rows, feats), vmem(7, feats, feats), vmem(3 + long_count, rows, grid_rows),
        pltpu.SMEM((2, *encode_live.shape), jnp.int32), pltpu.SMEM((2, *encode_groups.shape), jnp.int32),
        vmem(3 + long_count, rows, rows), vmem(*decode_near.shape),
        vmem(CHUNKS, grid_rows, width),
        vmem(CHUNKS, halves, *piece, dtype=F32), vmem(CHUNKS, far_count, halves, *piece),
        vmem(CHUNKS, halves, *piece), vmem(CHUNKS, far_count, halves, *piece),
        vmem(2, CHUNKS, *block), vmem(2, CHUNKS, *block),
        vmem(CHUNKS, *block), vmem(CHUNKS, far_count, *block), vmem(2, CHUNKS, *block),
        vmem(CHUNKS, *block), vmem(2, CHUNKS, *block),
        vmem(rows, feats), vmem(far_count, rows, rows),
        dma((10,)), dma((2,)), dma((CHUNKS + 1,)), dma((ODD_RS, halves)), dma((CHUNKS,)), dma((2,)), dma((2,)),
        dma((CHUNKS + 1,)), dma((ODD_AG, halves)), dma((CHUNKS, 2)), dma((2,)), dma((2,)), dma((2,)), dma((2, CHUNKS)), pltpu.SemaphoreType.REGULAR((2,)),
    ]
    hbm = pl.BlockSpec(memory_space=pltpu.HBM)
    on_chip = pl.BlockSpec(memory_space=pltpu.VMEM)
    held = pl.pallas_call(
        functools.partial(exchange, groups, devs),
        out_shape=(
            vmem(*mesh_state.shape), vmem(*grid_state.shape), vmem(2, feats, feats), vmem(*grid_state.shape, dtype=F32),
        ),
        in_specs=[hbm] * len(args),
        out_specs=(on_chip,) * 4,
        scratch_shapes=scratch,
        compiler_params=pltpu.CompilerParams(collective_id=0, has_side_effects=True, vmem_limit_bytes=32 << 20),
        name="exchange",
    )(*(pltpu.with_memory_space_constraint(arg, pltpu.HBM) for arg in args))
    return pl.pallas_call(
        finish,
        out_shape=(
            jax.ShapeDtypeStruct(grid_state.shape, BF16),
            jax.ShapeDtypeStruct(mesh_state.shape, BF16),
        ),
        in_specs=[on_chip] * 4,
        out_specs=(hbm, hbm),
        scratch_shapes=[vmem(*grid_state.shape), dma((1 + GRID_OUTS,))],
        compiler_params=pltpu.CompilerParams(vmem_limit_bytes=16 << 20),
        name="finish",
    )(*held)


def solution(mesh):
    both = ("group", "dev")
    row, whole, second = P(both, None), P(), P(None, both, None)
    flags = P(None, both)
    return jax.shard_map(
        functools.partial(body, mesh.shape["group"], mesh.shape["dev"]),
        mesh=mesh,
        in_specs=(
            row, row, whole, whole, whole, whole, whole, whole, whole, whole, whole,
            second, flags, second, flags, second, second, flags, second, flags,
        ),
        out_specs=(row, row),
        check_vma=False,
    )
```
